256 devices in a mesh: seq: 2 (over core), ctx: 32 (over x, z_hi, y), tp: 4 (over z_lo).
Axes of the slice: x: 4, y: 4, z: 8 (z_hi: 2, z_lo: 4; z = z_hi * 4 + z_lo), core: 2. Of those that a mesh axis runs over, the one named last changes fastest.
Arguments:
- queries: bfloat16 [16384, 16, 128], P(('seq', 'ctx'), 'tp'), parts along dimension 0, may hold values from -160 to 160
- key_rows: bfloat16 [16384, 4, 128], P(('seq', 'ctx'), 'tp'), parts along dimension 0, may hold values from -5 to 5
- value_slot_rows: bfloat16 [16384, 4, 128], P(('seq', 'ctx'), 'tp'), parts along dimension 0, may hold values from -6 to 6
- out_grad: bfloat16 [16384, 16, 128], P(('seq', 'ctx'), 'tp'), parts along dimension 0, may hold values from -6 to 6
- span_order: int32 [128], P('seq'), parts along dimension 0, may hold values from 0 to 63, each once
Outputs:
- query_grad: bfloat16 [16384, 16, 128], P(('seq', 'ctx'), 'tp'), parts along dimension 0
- key_gradient: bfloat16 [16384, 4, 128], P(('seq', 'ctx'), 'tp'), parts along dimension 0
- value_gradient: bfloat16 [16384, 4, 128], P(('seq', 'ctx'), 'tp'), parts along dimension 0
The draws below stay inside these ranges and needn't reach their ends.
There are 2 independent parts, one for each index of `seq`. The reference program is written for one: setup_inputs(seed, part) draws one part's arguments, and reference() takes and returns one part's arrays. A program takes and returns all parts, laid end to end along the dimension named above; each array names one. Nothing has to cross between parts.
Inputs may be any that keep to these rules, and one draw needn't show every extreme that they name: Slot s of 128 rows holds span span_order[s] of the sequence; every span number stands once.
All inputs are finite; a program needn't handle non-finite values.
Results may differ from the reference program's by a relative error of at most 0.0085.
Values may be sent and summed in bfloat16 or wider, within the bound.
A program may use at most 64 MiB of HBM per device.

```python
import math
import jax
import jax.numpy as jnp
from jax import lax

HEAD_SIZE = 128
QUERY_HEADS = 16
KEY_VALUE_HEADS = 4
SPAN = 128
SLOTS = 64
SEQUENCE_TOKENS = 8192


def keys_base(key):
    return jax.random.truncated_normal(jax.random.fold_in(key, 7), -5.0, 5.0, (SEQUENCE_TOKENS, KEY_VALUE_HEADS, HEAD_SIZE), jnp.float32)


def draw_key_rows(key, part):
    values = keys_base(key)
    return values.astype(jnp.bfloat16)


def draw_queries(key, part):
    values = jax.random.truncated_normal(jax.random.fold_in(key, 11), -5.0, 5.0, (SEQUENCE_TOKENS, QUERY_HEADS, HEAD_SIZE), jnp.float32)
    return values.astype(jnp.bfloat16)


def steps_of(key, extent, cuts, smallest, top_value):
    def one(position, shards_of):
        draws = jax.random.uniform(jax.random.fold_in(jax.random.fold_in(key, 6), position), (shards_of,), jnp.float32, smallest / len(cuts), top_value / len(cuts))
        return jnp.repeat(jnp.exp(draws), extent[position] // shards_of).reshape((-1,) + (1,) * (len(extent) - position - 1))

    loudness = one(*cuts[0])
    for cut in cuts[1:]:
        loudness = loudness * one(*cut)
    return loudness


def scatter_about(key, dims, spread, bound, pieces=(), held_as=jnp.bfloat16):
    result = spread * jax.random.normal(key, dims, jnp.float32)
    if pieces:
        result = result * steps_of(key, dims, pieces, -0.22, 0.18)
    return jnp.clip(result, -bound, bound).astype(held_as)


def setup_inputs(seed: int = 0, part: int = 0) -> dict:
    key_list = jax.random.split(jax.random.key(seed), 6)
    own_keys = jax.random.split(jax.random.fold_in(key_list[5], part), 6)
    return {
        "queries": draw_queries(jax.random.fold_in(jax.random.fold_in(key_list[5], part), 71), part),
        "key_rows": draw_key_rows(jax.random.fold_in(jax.random.fold_in(key_list[5], part), 71), part),
        "value_slot_rows": scatter_about(own_keys[2], (SEQUENCE_TOKENS, KEY_VALUE_HEADS, HEAD_SIZE), 1.0, 6.0, ((0, 32), (1, 4))),
        "out_grad": scatter_about(own_keys[3], (SEQUENCE_TOKENS, QUERY_HEADS, HEAD_SIZE), 1.0, 6.0, ((0, 32), (1, 4))),
        "span_order": jax.random.permutation(own_keys[4], SLOTS).astype(jnp.int32),
    }


NEGATIVE = -1e+30

def positions_of(span_order):
    offsets = jnp.tile(jnp.arange(SPAN, dtype=jnp.int32), SLOTS)
    return (jnp.repeat(span_order.astype(jnp.int32), SPAN) * SPAN + offsets).astype(jnp.int32)

def head_grads(query_head, key_head, value_head, grad_head, places):
    scaling = 1.0 / math.sqrt(HEAD_SIZE)
    value_wide = value_head.astype(jnp.float32)

    def step(carried, block_index):
        key_acc, value_acc = carried
        begin = (block_index * SPAN).astype(jnp.int32)
        q_block = lax.dynamic_slice_in_dim(query_head, begin, SPAN, 0)
        g_block = lax.dynamic_slice_in_dim(grad_head, begin, SPAN, 0)
        q_places = lax.dynamic_slice_in_dim(places, begin, SPAN, 0)
        visible = q_places[:, None] >= places[None, :]
        scores = jnp.dot(q_block, key_head.T, preferred_element_type=jnp.float32) * scaling
        scores = jnp.where(visible, scores, NEGATIVE)
        row_top = lax.optimization_barrier(jnp.max(scores, axis=1, keepdims=True))
        row_sum = lax.optimization_barrier(jnp.sum(jnp.where(visible, jnp.exp(scores - row_top), 0.0), axis=1, keepdims=True))
        log_total = row_top + jnp.log(row_sum)
        probs = jnp.where(visible, jnp.exp(scores - log_total), 0.0)
        probs_low = probs.astype(jnp.bfloat16)
        output = jnp.dot(probs, value_wide, precision=lax.Precision.HIGHEST, preferred_element_type=jnp.float32)
        row_delta = lax.optimization_barrier(jnp.sum(g_block.astype(jnp.float32) * output, axis=1, keepdims=True))
        grad_probs = jnp.dot(g_block, value_head.T, preferred_element_type=jnp.float32)
        grad_scores = (probs * (grad_probs - row_delta) * scaling).astype(jnp.bfloat16)
        query_part = jnp.dot(grad_scores, key_head, preferred_element_type=jnp.float32).astype(jnp.bfloat16)
        key_acc = key_acc + jnp.dot(grad_scores.T, q_block, preferred_element_type=jnp.float32)
        value_acc = value_acc + jnp.dot(probs_low.T, g_block, preferred_element_type=jnp.float32)
        return ((key_acc, value_acc), query_part)
    zeros = jnp.zeros((SEQUENCE_TOKENS, HEAD_SIZE), jnp.float32)
    (key_acc, value_acc), query_parts = lax.scan(step, (zeros, zeros), jnp.arange(SEQUENCE_TOKENS // SPAN, dtype=jnp.int32))
    return (query_parts.reshape(SEQUENCE_TOKENS, HEAD_SIZE), key_acc, value_acc)

def reference(queries, key_rows, value_slot_rows, out_grad, span_order):
    places = positions_of(span_order)
    query_cluster = QUERY_HEADS // KEY_VALUE_HEADS

    def per_head(head):
        kv_head = head // query_cluster
        query_head = lax.dynamic_index_in_dim(queries, head, 1, keepdims=False)
        grad_head = lax.dynamic_index_in_dim(out_grad, head, 1, keepdims=False)
        key_head = lax.dynamic_index_in_dim(key_rows, kv_head, 1, keepdims=False)
        value_head = lax.dynamic_index_in_dim(value_slot_rows, kv_head, 1, keepdims=False)
        return head_grads(query_head, key_head, value_head, grad_head, places)
    query_all, key_complete, value_complete = lax.map(per_head, jnp.arange(QUERY_HEADS, dtype=jnp.int32))
    query_grad = jnp.transpose(query_all, (1, 0, 2))
    key_gradient = jnp.transpose(key_complete.reshape(KEY_VALUE_HEADS, query_cluster, SEQUENCE_TOKENS, HEAD_SIZE).sum(axis=1), (1, 0, 2)).astype(jnp.bfloat16)
    value_gradient = jnp.transpose(value_complete.reshape(KEY_VALUE_HEADS, query_cluster, SEQUENCE_TOKENS, HEAD_SIZE).sum(axis=1), (1, 0, 2)).astype(jnp.bfloat16)
    return (query_grad, key_gradient, value_gradient)
```

```python
import functools
import math

import jax
import jax.numpy as jnp
from jax import lax
from jax.experimental import pallas as pl
from jax.experimental.pallas import tpu as pltpu
from jax.sharding import PartitionSpec as P

MESH = pl.DeviceIdType.MESH
SPAN = 128
HEADS = 4
DIM = 128
COLS = 2 * HEADS * SPAN
CHUNK = 4 * SPAN
HIDDEN = -1e30
F32 = jnp.float32
BF16 = jnp.bfloat16

CHUNKS = (
    ((1, 0), (3, 0)),
    ((0, 1), (0, 3)),
    ((0, 0), (2, 0)),
    ((1, 1), (1, 3)),
    ((3, 1), (3, 3)),
    ((2, 1), (2, 3)),
    ((1, 2), (3, 2)),
    ((0, 2), (2, 2)),
)
PLACE = {
    (da, db): (chunk, pos)
    for chunk, pair in enumerate(CHUNKS)
    for pos, (da, db) in enumerate(pair)
}


def slot_of(base, colour, da, db):
    chunk, pos = PLACE[(da % 4, db % 4)]
    return base + chunk * 4 + colour * 2 + pos


def kernel(
    span_ref, q_ref, g_ref, k_ref, v_ref,
    dq_ref, dk_ref, dv_ref,
    kv, part, stage, half_in, full_in, ring_in, z_in,
    qt, gt, qrows, grows, lhs, pbuf, dsbuf, dqt, top, total, delta, spans,
    load_sem, gather_send, gather_recv, gather_z, reduce_send, reduce_recv, reduce_z,
):
    me = lax.axis_index("ctx")
    x, z, y = me // 8, (me // 4) % 2, me % 4

    def at(xx, zz, yy):
        return (xx % 4) * 8 + (zz % 2) * 4 + yy % 4

    x_up, x_down = at(x + 1, z, y), at(x + 3, z, y)
    y_up, y_down = at(x, z, y + 1), at(x, z, y + 3)
    z_other = at(x, z + 1, y)
    ring_a = ((x_up, x_down), (y_up, y_down))
    ring_b = ((y_up, y_down), (x_up, x_down))

    loads = []
    for colour in range(2):
        own = slot_of(0, colour, 0, 0)
        rows = pl.ds(colour * SPAN, SPAN)
        loads.append(pltpu.make_async_copy(k_ref.at[rows], kv.at[own, 0], load_sem.at[2 * colour]))
        loads.append(
            pltpu.make_async_copy(v_ref.at[rows], kv.at[own, 1], load_sem.at[2 * colour + 1])
        )
    for copy in loads:
        copy.start()

    barrier = pltpu.get_barrier_semaphore()
    for other in (x_up, x_down, y_up, y_down, z_other):
        pl.semaphore_signal(barrier, inc=1, device_id={"ctx": other}, device_id_type=MESH)
    pl.semaphore_wait(barrier, 5)
    for copy in loads:
        copy.wait()

    def send(src, dst, send_sem, recv_sem, device):
        pltpu.make_async_remote_copy(
            src_ref=src, dst_ref=dst, send_sem=send_sem, recv_sem=recv_sem,
            device_id={"ctx": device}, device_id_type=MESH,
        ).start()

    def await_units(sem, units):
        block = kv.at[pl.ds(0, units)]
        pltpu.make_async_copy(block, block, sem).wait()

    def gather(dz, group, src, dst, device):
        send(src, dst, gather_send, gather_recv.at[dz, group], device)

    def gather_own(base, dz):
        for c in range(2):
            own = kv.at[slot_of(base, c, 0, 0)]
            gather(dz, 0, own, kv.at[slot_of(base, c, 3, 0)], ring_a[c][0])
            gather(dz, 0, own, kv.at[slot_of(base, c, 1, 0)], ring_a[c][1])
        gather_second(base, dz, 1, 0)

    def gather_second(base, dz, group, da):
        for c in range(2):
            unit = kv.at[slot_of(base, c, da, 0)]
            gather(dz, group, unit, kv.at[slot_of(base, c, da, 3)], ring_b[c][0])
            gather(dz, group, unit, kv.at[slot_of(base, c, da, 1)], ring_b[c][1])

    def gather_first_opposite(base, dz):
        for c in range(2):
            there = slot_of(base, c, 2, 0)
            gather(dz, 2, kv.at[slot_of(base, c, 3, 0), 0], kv.at[there, 0], ring_a[c][0])
            gather(dz, 2, kv.at[slot_of(base, c, 1, 0), 1], kv.at[there, 1], ring_a[c][1])

    def gather_second_opposite(base, dz, group, da):
        for c in range(2):
            there = slot_of(base, c, da, 2)
            gather(dz, group, kv.at[slot_of(base, c, da, 3), 0], kv.at[there, 0], ring_b[c][0])
            gather(dz, group, kv.at[slot_of(base, c, da, 1), 1], kv.at[there, 1], ring_b[c][1])

    for c in range(2):
        send(
            kv.at[slot_of(0, c, 0, 0)], kv.at[slot_of(32, c, 0, 0)],
            gather_send, gather_z, z_other,
        )
    gather_own(0, 0)

    for dz in range(2):
        for da in range(4):
            for db in range(4):
                for c in range(2):
                    dx, dy = (da, db) if c == 0 else (db, da)
                    owner = at(x + dx, z + dz, y + dy)
                    spans[slot_of(32 * dz, c, da, db)] = span_ref[owner * 2 + c]
    mine = [span_ref[me * 2 + s] for s in range(2)]

    lane = lax.broadcasted_iota(jnp.int32, (SPAN, SPAN), 1)
    sublane = lax.broadcasted_iota(jnp.int32, (SPAN, SPAN), 0)
    identity = jnp.where(lane == sublane, 1.0, 0.0).astype(BF16)
    for s in range(2):
        for h in range(HEADS):
            rows = pl.ds(s * SPAN, SPAN)
            heads = pl.ds(h * DIM, DIM)
            here = pl.ds((s * HEADS + h) * SPAN, SPAN)
            q_block, g_block = q_ref[rows, heads], g_ref[rows, heads]
            qrows[here, :] = q_block
            grows[here, :] = g_block
            qt[0:DIM, here] = q_block.astype(F32).T.astype(BF16)
            gt[:, here] = g_block.astype(F32).T.astype(BF16)
            qt[DIM : 2 * DIM, here] = identity
    top[...] = jnp.full_like(top, HIDDEN)
    total[...] = jnp.zeros_like(total)
    delta[...] = jnp.zeros_like(delta)
    dqt[...] = jnp.zeros_like(dqt)

    exponent = math.log2(math.e) / math.sqrt(DIM)

    def load_chunk(chunk):
        keys = kv[pl.ds(chunk * 4, 4), 0].reshape(CHUNK, DIM)
        values = kv[pl.ds(chunk * 4, 4), 1].reshape(CHUNK, DIM)
        ahead = sublane - lane
        for s in range(2):
            lhs[s, :, 0:DIM] = keys
            for u in range(4):
                limit = (mine[s] - spans[chunk * 4 + u]) * SPAN
                lhs[s, u * SPAN : (u + 1) * SPAN, DIM : 2 * DIM] = jnp.where(
                    ahead > limit, HIDDEN, 0.0
                ).astype(BF16)
        return keys, values

    WIDE = 256
    TILES = COLS // WIDE

    def scores(tile):
        cols = pl.ds(tile * WIDE, WIDE)
        s = tile * WIDE // (HEADS * SPAN)
        return cols, jnp.dot(lhs[s], qt[:, cols], preferred_element_type=F32)

    def fold(values, op):
        return op(values.reshape(CHUNK // 8, 8, WIDE), axis=0)

    def forward(chunk, _):
        dz, step = chunk // 8, chunk % 8
        base = dz * 32

        @pl.when(step == 0)
        def _():
            await_units(gather_recv.at[dz, 0], 4)
            gather_first_opposite(base, dz)
            gather_second(base, dz, 3, 1)
            gather_second(base, dz, 4, 3)

        @pl.when(step == 1)
        def _():
            await_units(gather_recv.at[dz, 1], 4)
            gather_second_opposite(base, dz, 6, 0)

        @pl.when(step == 2)
        def _():
            await_units(gather_recv.at[dz, 2], 2)
            gather_second(base, dz, 5, 2)

        @pl.when(step == 3)
        def _():
            await_units(gather_recv.at[dz, 3], 4)
            gather_second_opposite(base, dz, 7, 1)

        @pl.when(step == 4)
        def _():
            await_units(gather_recv.at[dz, 4], 4)
            gather_second_opposite(base, dz, 8, 3)

        @pl.when(step == 5)
        def _():
            await_units(gather_recv.at[dz, 5], 4)
            gather_second_opposite(base, dz, 9, 2)

        @pl.when(chunk == 6)
        def _():
            await_units(gather_z, 2)
            gather_own(32, 1)

        @pl.when(step == 6)
        def _():
            await_units(gather_recv.at[dz, 7], 2)
            await_units(gather_recv.at[dz, 8], 2)

        @pl.when(step == 7)
        def _():
            await_units(gather_recv.at[dz, 6], 2)
            await_units(gather_recv.at[dz, 9], 2)

        keys, values = load_chunk(chunk)
        for tile in range(TILES):
            cols, score = scores(tile)
            grad_probs = jnp.dot(values, gt[:, cols], preferred_element_type=F32)
            before = top[:, cols]
            now = jnp.maximum(before, jnp.max(fold(score, jnp.max), axis=0, keepdims=True))
            rescale = jnp.exp2((before - now) * exponent)
            weights = jnp.exp2((score - now) * exponent)
            top[:, cols] = now
            total[:, cols] = total[:, cols] * rescale + fold(weights, jnp.sum)
            delta[:, cols] = delta[:, cols] * rescale + fold(weights * grad_probs, jnp.sum)
        return 0

    lax.fori_loop(0, 16, forward, 0)

    weight = jnp.sum(total[...], axis=0, keepdims=True)
    row_delta = jnp.sum(delta[...], axis=0, keepdims=True) / weight
    top[...] = top[...] + jnp.log(weight) * math.sqrt(DIM)
    delta[0:1, :] = row_delta

    def reduce(dz, group, src, dst, device):
        send(src, dst, reduce_send, reduce_recv.at[dz, group], device)

    def send_halves(base, dz, da):
        for c in range(2):
            slot = slot_of(base, c, da, 2)
            stage[slot] = part[slot].astype(BF16)
            up, down = ring_b[c]
            reduce(dz, da, stage.at[slot, 0], half_in.at[slot_of(base, c, da, 1)], up)
            reduce(dz, da, stage.at[slot, 1], half_in.at[slot_of(base, c, da, 3)], down)

    def add_half(slot, which, sums):
        arrived = half_in[slot].astype(F32)
        return [sums[0] + arrived, sums[1]] if which == 0 else [sums[0], sums[1] + arrived]

    def put(slot, sums):
        stage[slot, 0] = sums[0].astype(BF16)
        stage[slot, 1] = sums[1].astype(BF16)

    def send_second(base, dz, da):
        await_units(reduce_recv.at[dz, da], 2)
        for c in range(2):
            for way, db in enumerate((1, 3)):
                slot = slot_of(base, c, da, db)
                put(slot, add_half(slot, way, [part[slot, 0], part[slot, 1]]))
                reduce(dz, 4 + da, stage.at[slot], full_in.at[dz, da, c, way], ring_b[c][way])

    def second_sum(base, dz, c, da):
        slot = slot_of(base, c, da, 0)
        return slot, [
            part[slot, i]
            + full_in[dz, da, c, 0, i].astype(F32)
            + full_in[dz, da, c, 1, i].astype(F32)
            for i in range(2)
        ]

    def send_first_halves(base, dz):
        await_units(reduce_recv.at[dz, 6], 4)
        for c in range(2):
            slot, sums = second_sum(base, dz, c, 2)
            put(slot, sums)
            up, down = ring_a[c]
            reduce(dz, 8, stage.at[slot, 0], half_in.at[slot_of(base, c, 1, 0)], up)
            reduce(dz, 8, stage.at[slot, 1], half_in.at[slot_of(base, c, 3, 0)], down)

    def send_first(base, dz):
        await_units(reduce_recv.at[dz, 5], 4)
        await_units(reduce_recv.at[dz, 7], 4)
        await_units(reduce_recv.at[dz, 8], 2)
        for c in range(2):
            for way, da in enumerate((1, 3)):
                slot, sums = second_sum(base, dz, c, da)
                put(slot, add_half(slot, way, sums))
                reduce(dz, 9, stage.at[slot], ring_in.at[dz, c, way], ring_a[c][way])

    def own_sum(base, dz, c):
        slot, sums = second_sum(base, dz, c, 0)
        return slot, [
            sums[i] + ring_in[dz, c, 0, i].astype(F32) + ring_in[dz, c, 1, i].astype(F32)
            for i in range(2)
        ]

    scaling = 1.0 / math.sqrt(DIM)

    def backward(turn, _):
        chunk = 15 - turn
        dz, step = 1 - turn // 8, turn % 8
        base = dz * 32
        keys, values = load_chunk(chunk)
        for tile in range(TILES):
            cols, score = scores(tile)
            grad_probs = jnp.dot(values, gt[:, cols], preferred_element_type=F32)
            probs = jnp.exp2((score - top[:, cols]) * exponent)
            pbuf[:, cols] = probs.astype(BF16)
            dsbuf[:, cols] = (probs * (grad_probs - delta[0:1, cols])).astype(BF16)
        grad_scores = dsbuf[...]
        value_part = jnp.dot(pbuf[...], grows[...], preferred_element_type=F32)
        key_part = jnp.dot(grad_scores, qrows[...], preferred_element_type=F32) * scaling
        part[pl.ds(chunk * 4, 4), 1] = value_part.reshape(4, SPAN, DIM)
        part[pl.ds(chunk * 4, 4), 0] = key_part.reshape(4, SPAN, DIM)
        keys_t = keys.astype(F32).T.astype(BF16)
        dqt[...] += jnp.dot(keys_t, grad_scores, preferred_element_type=F32)

        @pl.when(step == 0)
        def _():
            send_halves(base, dz, 0)
            send_halves(base, dz, 2)

        @pl.when(step == 1)
        def _():
            send_halves(base, dz, 1)
            send_halves(base, dz, 3)

        @pl.when(step == 3)
        def _():
            send_second(base, dz, 2)

        @pl.when(step == 4)
        def _():
            send_second(base, dz, 3)

        @pl.when(step == 5)
        def _():
            send_second(base, dz, 1)

        @pl.when(step == 6)
        def _():
            send_first_halves(base, dz)
            send_second(base, dz, 0)

        @pl.when(turn == 8)
        def _():
            send_first(32, 1)

        @pl.when(turn == 10)
        def _():
            await_units(reduce_recv.at[1, 4], 4)
            await_units(reduce_recv.at[1, 9], 4)
            for c in range(2):
                slot, sums = own_sum(32, 1, c)
                put(slot, sums)
                send(stage.at[slot], z_in.at[c], reduce_send, reduce_z, z_other)

        return 0

    lax.fori_loop(0, 16, backward, 0)

    send_first(0, 0)
    for s in range(2):
        for h in range(HEADS):
            here = pl.ds((s * HEADS + h) * SPAN, SPAN)
            dq_ref[pl.ds(s * SPAN, SPAN), pl.ds(h * DIM, DIM)] = (
                (dqt[:, here] * scaling).T.astype(BF16)
            )
    await_units(reduce_recv.at[0, 4], 4)
    await_units(reduce_z, 2)
    await_units(reduce_recv.at[0, 9], 4)
    for c in range(2):
        _, sums = own_sum(0, 0, c)
        rows = pl.ds(c * SPAN, SPAN)
        dk_ref[rows, :] = (sums[0] + z_in[c, 0].astype(F32)).astype(BF16)
        dv_ref[rows, :] = (sums[1] + z_in[c, 1].astype(F32)).astype(BF16)
    await_units(gather_send, 62)
    await_units(reduce_send, 62)


def local(queries, key_rows, value_slot_rows, out_grad, span_order):
    rows = queries.shape[0]
    vmem = pl.BlockSpec(memory_space=pltpu.VMEM)
    unit = (2, SPAN, DIM)
    dma = pltpu.SemaphoreType.DMA
    dq, dk, dv = pl.pallas_call(
        kernel,
        out_shape=(
            jax.ShapeDtypeStruct((rows, HEADS * DIM), BF16),
            jax.ShapeDtypeStruct((rows, DIM), BF16),
            jax.ShapeDtypeStruct((rows, DIM), BF16),
        ),
        in_specs=[
            pl.BlockSpec(memory_space=pltpu.SMEM), vmem, vmem,
            pl.BlockSpec(memory_space=pl.ANY), pl.BlockSpec(memory_space=pl.ANY),
        ],
        out_specs=(vmem, vmem, vmem),
        scratch_shapes=[
            pltpu.VMEM((64,) + unit, BF16),
            pltpu.VMEM((64,) + unit, F32),
            pltpu.VMEM((64,) + unit, BF16),
            pltpu.VMEM((64, SPAN, DIM), BF16),
            pltpu.VMEM((2, 4, 2, 2) + unit, BF16),
            pltpu.VMEM((2, 2, 2) + unit, BF16),
            pltpu.VMEM((2,) + unit, BF16),
            pltpu.VMEM((2 * DIM, COLS), BF16),
            pltpu.VMEM((DIM, COLS), BF16),
            pltpu.VMEM((COLS, DIM), BF16),
            pltpu.VMEM((COLS, DIM), BF16),
            pltpu.VMEM((2, CHUNK, 2 * DIM), BF16),
            pltpu.VMEM((CHUNK, COLS), BF16),
            pltpu.VMEM((CHUNK, COLS), BF16),
            pltpu.VMEM((DIM, COLS), F32),
            pltpu.VMEM((1, COLS), F32),
            pltpu.VMEM((8, COLS), F32),
            pltpu.VMEM((8, COLS), F32),
            pltpu.SMEM((64,), jnp.int32),
            dma((4,)), dma, dma((2, 10)), dma, dma, dma((2, 10)), dma,
        ],
        compiler_params=pltpu.CompilerParams(
            collective_id=0, has_side_effects=True, vmem_limit_bytes=60 * 1024 * 1024,
        ),
    )(
        span_order,
        queries.reshape(rows, HEADS * DIM),
        out_grad.reshape(rows, HEADS * DIM),
        key_rows.reshape(rows, DIM),
        value_slot_rows.reshape(rows, DIM),
    )
    return (
        dq.reshape(rows, HEADS, DIM),
        dk.reshape(rows, 1, DIM),
        dv.reshape(rows, 1, DIM),
    )


def solution(mesh):
    row = P(("seq", "ctx"), "tp", None)
    return jax.shard_map(
        local,
        mesh=mesh,
        in_specs=(row, row, row, row, P("seq")),
        out_specs=(row, row, row),
        check_vma=False,
    )
```

```python
import math

import jax
import jax.numpy as jnp
from jax import lax
from jax.experimental import pallas as pl
from jax.experimental.pallas import tpu as pltpu
from jax.sharding import PartitionSpec as P

MESH = pl.DeviceIdType.MESH
SPAN = 128
HEADS = 4
DIM = 128
COLS = 2 * HEADS * SPAN
CHUNK = 4 * SPAN
WIDE = 256
TILES = COLS // WIDE
BLOCK = 64
HIDDEN = -1e30
F32 = jnp.float32
BF16 = jnp.bfloat16

CHUNKS = (
    ((0, 0, 0), (1, 0, 0), (0, 1, 0), (0, 3, 0)),
    ((0, 0, 1), (1, 0, 1), (1, 1, 0), (1, 3, 0)),
    ((0, 1, 1), (0, 3, 1), (1, 1, 1), (1, 3, 1)),
    ((0, 2, 0), (1, 2, 0), (0, 2, 1), (1, 2, 1)),
)
FORWARD = (
    (0, 0), (1, 0), (2, 0), (3, 0), (4, 0), (0, 1), (1, 1), (2, 1),
    (3, 1), (5, 0), (4, 1), (5, 1), (6, 0), (6, 1), (7, 0), (7, 1),
)
BACKWARD = (
    (7, 1), (7, 0), (6, 1), (6, 0), (5, 1), (5, 0), (4, 1), (4, 0),
    (3, 1), (3, 0), (2, 1), (2, 0), (1, 1), (0, 1), (1, 0), (0, 0),
)
PLACE = {unit: 4 * i + j for i, units in enumerate(CHUNKS) for j, unit in enumerate(units)}


def pick(step, values):
    return sum(jnp.where(step == i, v, 0) for i, v in enumerate(values) if v)


def when(condition):
    def run(body):
        lax.fori_loop(0, condition.astype(jnp.int32), lambda _, c: (body(), c)[1], 0)

    return run


def kernel(
    span_ref, q_ref, g_ref, k_ref, v_ref,
    dq_ref, dk_ref, dv_ref,
    kv, part, stage, half_in, x_in, e_in, z_in, dq_out, dq_in,
    qt, gt, qrows, grows, lhs, pbuf, dsbuf, dqt, top, total, delta, stats_out, stats_in,
    spans, own_spans,
    load_sem, gather_send, gather_recv, gather_z, q_send, q_recv, stat_send, stat_recv,
    reduce_send, reduce_recv, reduce_z, dq_send, dq_recv,
):
    me = lax.axis_index("ctx")
    x, z, y = me // 8, (me // 4) % 2, me % 4

    def at(xx, zz, yy):
        return (xx % 4) * 8 + (zz % 2) * 4 + yy

    x_ways = (at(x + 1, z, y), at(x + 3, z, y))
    partner = at(x, z, y + 1 - 2 * (y % 2))
    other = at(x, z, 3 - y)
    z_other = at(x, z + 1, y)

    def slot_of(base, c, da, e):
        return base + PLACE[(c, da, e)]

    loads = []
    for c in range(2):
        own = slot_of(0, c, 0, 0)
        rows = pl.ds(c * SPAN, SPAN)
        loads.append(pltpu.make_async_copy(k_ref.at[rows], kv.at[own, 0], load_sem.at[2 * c]))
        loads.append(pltpu.make_async_copy(v_ref.at[rows], kv.at[own, 1], load_sem.at[2 * c + 1]))
    loads.append(pltpu.make_async_copy(q_ref, qrows.at[0], load_sem.at[4]))
    loads.append(pltpu.make_async_copy(g_ref, grows.at[0], load_sem.at[5]))
    for copy in loads:
        copy.start()

    barrier = pltpu.get_barrier_semaphore()
    for device in (*x_ways, partner, other, z_other):
        pl.semaphore_signal(barrier, inc=1, device_id={"ctx": device}, device_id_type=MESH)
    pl.semaphore_wait(barrier, 5)
    for copy in loads:
        copy.wait()

    def send(src, dst, send_sem, recv_sem, device):
        pltpu.make_async_remote_copy(
            src_ref=src, dst_ref=dst, send_sem=send_sem, recv_sem=recv_sem,
            device_id={"ctx": device}, device_id_type=MESH,
        ).start()

    def await_units(sem, units):
        block = kv.at[pl.ds(0, units)]
        pltpu.make_async_copy(block, block, sem).wait()

    def gather(dz, group, src, dst, device):
        send(src, dst, gather_send, gather_recv.at[dz, group], device)

    def arrived(dz, *groups):
        for group in groups:
            await_units(gather_recv.at[dz, group], (1, 2, 1, 2, 1, 1, 2, 1, 2, 1)[group])

    def along_x(dz, group, c, e):
        unit = kv.at[slot_of(16 * dz, c, 0, e)]
        gather(dz, group, unit, kv.at[slot_of(16 * dz, c, 3, e)], x_ways[0])
        gather(dz, group, unit, kv.at[slot_of(16 * dz, c, 1, e)], x_ways[1])

    def opposite_x(dz, group, c, e):
        there, up, down = (slot_of(16 * dz, c, da, e) for da in (2, 3, 1))
        gather(dz, group, kv.at[up, 0], kv.at[there, 0], x_ways[0])
        gather(dz, group, kv.at[down, 1], kv.at[there, 1], x_ways[1])

    def across(dz, group, c, da):
        src, dst = slot_of(16 * dz, c, da, 0), slot_of(16 * dz, c, da, 1)
        gather(dz, group, kv.at[src], kv.at[dst], other)

    def gather_own(dz):
        along_x(dz, 1, 0, 0)
        across(dz, 0, 0, 0)
        along_x(dz, 8, 1, 0)
        across(dz, 5, 1, 0)

    def gather_a(dz):
        arrived(dz, 1)
        opposite_x(dz, 2, 0, 0)
        arrived(dz, 0)
        along_x(dz, 3, 0, 1)

    def gather_b(dz):
        arrived(dz, 8)
        opposite_x(dz, 9, 1, 0)
        across(dz, 6, 1, 1)
        across(dz, 6, 1, 3)

    def gather_c(dz):
        arrived(dz, 9)
        across(dz, 7, 1, 2)
        arrived(dz, 3)
        opposite_x(dz, 4, 0, 1)

    for c in range(2):
        send(
            kv.at[slot_of(0, c, 0, 0)], kv.at[slot_of(16, c, 0, 0)],
            gather_send, gather_z, z_other,
        )
    gather_own(0)
    send(qrows.at[0], qrows.at[1], q_send, q_recv, partner)
    send(grows.at[0], grows.at[1], q_send, q_recv, partner)

    for dz in range(2):
        for c, da, e in PLACE:
            owner = at(x + da, z + dz, y if e == 0 else 3 - y)
            spans[slot_of(16 * dz, c, da, e)] = span_ref[owner * 2 + c]
    for group, device in enumerate((me, partner)):
        for s in range(2):
            own_spans[group * 2 + s] = span_ref[device * 2 + s]

    lane = lax.broadcasted_iota(jnp.int32, (SPAN, SPAN), 1)
    sublane = lax.broadcasted_iota(jnp.int32, (SPAN, SPAN), 0)

    def prepare(group):
        for block in range(COLS // SPAN):
            here = pl.ds(block * SPAN, SPAN)
            qt[group, 0:DIM, here] = qrows[group, here, :].astype(F32).T.astype(BF16)
            gt[group, :, here] = grows[group, here, :].astype(F32).T.astype(BF16)
            row = block % HEADS * (SPAN // HEADS) + lane // HEADS
            qt[group, DIM : 2 * DIM, here] = jnp.where(row == sublane, 1.0, 0.0).astype(BF16)

    prepare(0)
    top[...] = jnp.full_like(top, HIDDEN)
    total[...] = jnp.zeros_like(total)
    delta[...] = jnp.zeros_like(delta)
    dqt[...] = jnp.zeros_like(dqt)

    exponent = math.log2(math.e) / math.sqrt(DIM)
    scaling = 1.0 / math.sqrt(DIM)

    def masked_keys(chunk, keys, group):
        ahead = sublane - lane
        for s in range(2):
            lhs[s, :, 0:DIM] = keys
            for u in range(4):
                limit = (own_spans[group * 2 + s] - spans[chunk * 4 + u]) * SPAN
                lhs[s, u * SPAN : (u + 1) * SPAN, DIM : 2 * DIM] = jnp.where(
                    ahead > limit, HIDDEN, 0.0
                ).astype(BF16)

    def load_chunk(chunk):
        keys = kv[pl.ds(chunk * 4, 4), 0].reshape(CHUNK, DIM)
        values = kv[pl.ds(chunk * 4, 4), 1].reshape(CHUNK, DIM)
        return keys, values

    def fold(values, op):
        return op(values.reshape(values.shape[0] // 8, 8, WIDE), axis=0)

    def partials(group):
        stats_out[group, :, 0:COLS] = top[group]
        stats_out[group, :, COLS : 2 * COLS] = jnp.sum(total[group], axis=0, keepdims=True)
        stats_out[group, :, 2 * COLS :] = jnp.sum(delta[group], axis=0, keepdims=True)
        send(
            stats_out.at[group], stats_in.at[1 - group],
            stat_send.at[group], stat_recv.at[1 - group], partner,
        )

    def combine(group):
        here, there = stats_out.at[group], stats_in.at[group]
        pltpu.make_async_copy(there, there, stat_recv.at[group]).wait()
        first, second, third = (pl.ds(i * COLS, COLS) for i in range(3))
        highest = jnp.maximum(here[:, first], there[:, first])
        a = jnp.exp2((here[:, first] - highest) * exponent)
        b = jnp.exp2((there[:, first] - highest) * exponent)
        weight = here[:, second] * a + there[:, second] * b
        top[group] = highest + jnp.log(weight) * math.sqrt(DIM)
        delta[group, 0:1, :] = (here[:, third] * a + there[:, third] * b) / weight

    def tile_of(tile):
        return pl.ds(tile * WIDE, WIDE), tile * WIDE // (HEADS * SPAN)

    def scores(group, tile):
        cols, s = tile_of(tile)
        return jnp.dot(lhs[s], qt[group, :, cols], preferred_element_type=F32)

    def forward(step, _):
        chunk = pick(step, [c for c, _ in FORWARD])
        group = pick(step, [g for _, g in FORWARD])

        @when(step == 0)
        def _():
            gather_a(0)

        @when(step == 1)
        def _():
            gather_b(0)
            arrived(0, 5)

        @when(step == 2)
        def _():
            gather_c(0)
            await_units(gather_z, 2)
            gather_own(1)
            arrived(0, 6)

        @when(step == 3)
        def _():
            arrived(0, 2, 4, 7)

        @when(step == 4)
        def _():
            gather_a(1)

        @when(step == 5)
        def _():
            await_units(q_recv, 8)
            prepare(1)

        @when(step == 6)
        def _():
            gather_b(1)

        @when(step == 9)
        def _():
            gather_c(1)
            arrived(1, 5)

        @when(step == 12)
        def _():
            arrived(1, 6)

        @when(step == 14)
        def _():
            arrived(1, 2, 4, 7)

        @when(step == 15)
        def _():
            partials(0)

        keys, values = load_chunk(chunk)

        def grads(tile):
            cols, _ = tile_of(tile)
            return jnp.dot(values, gt[group, :, cols], preferred_element_type=F32)

        def topped(tile):
            cols, _ = tile_of(tile)
            score = scores(group, tile)
            before = top[group, :, cols]
            now = jnp.maximum(before, jnp.max(fold(score, jnp.max), axis=0, keepdims=True))
            top[group, :, cols] = now
            return score, now, jnp.exp2((before - now) * exponent)

        masked_keys(chunk, keys, group)
        ahead = topped(0)
        for tile in range(TILES):
            cols, _ = tile_of(tile)
            score, now, rescale = ahead
            if tile + 1 < TILES:
                ahead = topped(tile + 1)
            grad_probs = grads(tile)
            weight = total[group, :, cols] * rescale
            product = delta[group, :, cols] * rescale
            for row in range(0, CHUNK, BLOCK):
                weights = jnp.exp2((score[row : row + BLOCK] - now) * exponent)
                weight += fold(weights, jnp.sum)
                product += fold(weights * grad_probs[row : row + BLOCK], jnp.sum)
            total[group, :, cols] = weight
            delta[group, :, cols] = product
        return 0

    lax.fori_loop(0, 16, forward, 0)
    partials(1)
    combine(1)

    def reduce(dz, group, src, dst, device):
        send(src, dst, reduce_send, reduce_recv.at[dz, group], device)

    def put(slot, sums):
        stage[slot, 0] = sums[0].astype(BF16)
        stage[slot, 1] = sums[1].astype(BF16)

    def partial_of(slot):
        return [part[slot, 0], part[slot, 1]]

    def plus(sums, ref):
        return [sums[i] + ref[i].astype(F32) for i in range(2)]

    def plus_half(sums, slot, which):
        arrived = half_in[slot].astype(F32)
        return [sums[0] + arrived, sums[1]] if which == 0 else [sums[0], sums[1] + arrived]

    def halves(base, dz, group, c, e, sums):
        slot = slot_of(base, c, 2, e)
        put(slot, sums)
        reduce(dz, group, stage.at[slot, 0], half_in.at[slot_of(base, c, 1, e)], x_ways[0])
        reduce(dz, group, stage.at[slot, 1], half_in.at[slot_of(base, c, 3, e)], x_ways[1])

    def sum_along_x(base, dz, group, c, e, kind, way, sums):
        slot = slot_of(base, c, (1, 3)[way], e)
        put(slot, plus_half(sums, slot, way))
        reduce(dz, group, stage.at[slot], x_in.at[dz, kind, way], x_ways[way])

    def sum_across(base, dz, group, c, da, place, sums):
        slot = slot_of(base, c, da, 1)
        put(slot, sums)
        reduce(dz, group, stage.at[slot], e_in.at[dz, place], other)

    def landed(dz, *groups):
        for group in groups:
            await_units(reduce_recv.at[dz, group], (1, 1, 2, 2, 1, 2, 2, 1, 1, 1)[group])

    def reduce_d(dz):
        base = 16 * dz
        halves(base, dz, 9, 0, 0, partial_of(slot_of(base, 0, 2, 0)))
        halves(base, dz, 0, 0, 1, partial_of(slot_of(base, 0, 2, 1)))
        sum_across(base, dz, 1, 1, 2, 2, partial_of(slot_of(base, 1, 2, 1)))

    def reduce_c(dz):
        base = 16 * dz
        for da in (1, 3):
            sum_across(base, dz, 3, 1, da, da, partial_of(slot_of(base, 1, da, 1)))
        landed(dz, 0)
        for way, da in enumerate((1, 3)):
            sum_along_x(base, dz, 2, 0, 1, 1, way, partial_of(slot_of(base, 0, da, 1)))

    def reduce_c_opposite(dz):
        base = 16 * dz
        landed(dz, 1)
        halves(base, dz, 4, 1, 0, plus(partial_of(slot_of(base, 1, 2, 0)), e_in.at[dz, 2]))

    def reduce_b(dz):
        base = 16 * dz
        sum_across(base, dz, 8, 1, 0, 0, partial_of(slot_of(base, 1, 0, 1)))
        landed(dz, 2)
        sums = partial_of(slot_of(base, 0, 0, 1))
        for way in range(2):
            sums = plus(sums, x_in.at[dz, 1, way])
        sum_across(base, dz, 7, 0, 0, 4, sums)
        landed(dz, 3, 4)
        for way, da in enumerate((1, 3)):
            sums = plus(partial_of(slot_of(base, 1, da, 0)), e_in.at[dz, da])
            sum_along_x(base, dz, 6, 1, 0, 2, way, sums)

    def reduce_a(dz):
        base = 16 * dz
        landed(dz, 9)
        for way, da in enumerate((1, 3)):
            sum_along_x(base, dz, 5, 0, 0, 0, way, partial_of(slot_of(base, 0, da, 0)))

    def own_sums(dz):
        landed(dz, 7, 8, 6, 5)
        for c in range(2):
            slot = slot_of(16 * dz, c, 0, 0)
            sums = partial_of(slot)
            for way in range(2):
                sums = plus(sums, x_in.at[dz, 2 * c, way])
            yield c, slot, plus(sums, e_in.at[dz, 4 - 4 * c])

    def query_grads(group):
        for block in range(COLS // SPAN):
            here = pl.ds(block * SPAN, SPAN)
            yield here, (dqt[group, :, here] * scaling).T

    def backward(step, _):
        chunk = pick(step, [c for c, _ in BACKWARD])
        group = pick(step, [g for _, g in BACKWARD])

        @when(step == 1)
        def _():
            combine(0)

        keys, values = load_chunk(chunk)
        masked_keys(chunk, keys, group)
        for tile in range(TILES):
            cols, _ = tile_of(tile)
            score = scores(group, tile)
            grad_probs = jnp.dot(values, gt[group, :, cols], preferred_element_type=F32)
            lse, mean = top[group, :, cols], delta[group, 0:1, cols]
            for row in range(0, CHUNK, BLOCK):
                rows = slice(row, row + BLOCK)
                probs = jnp.exp2((score[rows] - lse) * exponent)
                pbuf[rows, cols] = probs.astype(BF16)
                dsbuf[rows, cols] = (probs * (grad_probs[rows] - mean)).astype(BF16)
        units = pl.ds(chunk * 4, 4)
        value_part = jnp.dot(pbuf[...], grows[group], preferred_element_type=F32)
        key_part = jnp.dot(dsbuf[...], qrows[group], preferred_element_type=F32) * scaling
        for which, found in ((1, value_part), (0, key_part)):
            before = jnp.where(group == 1, 0.0, part[units, which])
            part[units, which] = before + found.reshape(4, SPAN, DIM)
        keys_t = keys.astype(F32).T.astype(BF16)
        dqt[group] += jnp.dot(keys_t, dsbuf[...], preferred_element_type=F32)

        events = (
            (1, 9, reduce_d), (3, 11, reduce_c), (4, 12, reduce_c_opposite), (6, 14, reduce_b),
        )
        for early, late, event in events:

            @when((step == early) | (step == late))
            def _():
                event(jnp.where(step < 8, 1, 0))

        @when(step == 7)
        def _():
            reduce_a(1)

        @when(step == 10)
        def _():
            for c, slot, sums in own_sums(1):
                put(slot, sums)
                send(stage.at[slot], z_in.at[c], reduce_send, reduce_z, z_other)

        @when(step == 13)
        def _():
            for here, block in query_grads(1):
                dq_out[here, :] = block.astype(BF16)
            send(dq_out, dq_in, dq_send, dq_recv, partner)

        return 0

    lax.fori_loop(0, 16, backward, 0)
    reduce_a(0)
    await_units(reduce_z, 2)
    for c, _, sums in own_sums(0):
        rows = pl.ds(c * SPAN, SPAN)
        dk_ref[rows, :] = (sums[0] + z_in[c, 0].astype(F32)).astype(BF16)
        dv_ref[rows, :] = (sums[1] + z_in[c, 1].astype(F32)).astype(BF16)
    await_units(dq_recv, 4)
    for here, block in query_grads(0):
        dq_ref[here, :] = (block + dq_in[here, :].astype(F32)).astype(BF16)
    await_units(gather_send, 30)
    await_units(q_send, 8)
    await_units(reduce_send, 30)
    await_units(dq_send, 4)
    for group in range(2):
        sent = stats_out.at[group]
        pltpu.make_async_copy(sent, sent, stat_send.at[group]).wait()


def local(queries, key_rows, value_slot_rows, out_grad, span_order):
    rows = queries.shape[0]
    vmem = pl.BlockSpec(memory_space=pltpu.VMEM)
    unit = (2, SPAN, DIM)
    dma = pltpu.SemaphoreType.DMA
    dq, dk, dv = pl.pallas_call(
        kernel,
        out_shape=(
            jax.ShapeDtypeStruct((rows * HEADS, DIM), BF16),
            jax.ShapeDtypeStruct((rows, DIM), BF16),
            jax.ShapeDtypeStruct((rows, DIM), BF16),
        ),
        in_specs=[
            pl.BlockSpec(memory_space=pltpu.SMEM),
            *([pl.BlockSpec(memory_space=pl.ANY)] * 4),
        ],
        out_specs=(vmem, vmem, vmem),
        scratch_shapes=[
            pltpu.VMEM((32,) + unit, BF16),
            pltpu.VMEM((32,) + unit, F32),
            pltpu.VMEM((32,) + unit, BF16),
            pltpu.VMEM((32, SPAN, DIM), BF16),
            pltpu.VMEM((2, 3, 2) + unit, BF16),
            pltpu.VMEM((2, 5) + unit, BF16),
            pltpu.VMEM((2,) + unit, BF16),
            pltpu.VMEM((COLS, DIM), BF16),
            pltpu.VMEM((COLS, DIM), BF16),
            pltpu.VMEM((2, 2 * DIM, COLS), BF16),
            pltpu.VMEM((2, DIM, COLS), BF16),
            pltpu.VMEM((2, COLS, DIM), BF16),
            pltpu.VMEM((2, COLS, DIM), BF16),
            pltpu.VMEM((2, CHUNK, 2 * DIM), BF16),
            pltpu.VMEM((CHUNK, COLS), BF16),
            pltpu.VMEM((CHUNK, COLS), BF16),
            pltpu.VMEM((2, DIM, COLS), F32),
            pltpu.VMEM((2, 1, COLS), F32),
            pltpu.VMEM((2, 8, COLS), F32),
            pltpu.VMEM((2, 8, COLS), F32),
            pltpu.VMEM((2, 1, 3 * COLS), F32),
            pltpu.VMEM((2, 1, 3 * COLS), F32),
            pltpu.SMEM((32,), jnp.int32),
            pltpu.SMEM((4,), jnp.int32),
            dma((6,)), dma, dma((2, 10)), dma, dma, dma, dma((2,)), dma((2,)),
            dma, dma((2, 10)), dma, dma, dma,
        ],
        compiler_params=pltpu.CompilerParams(
            collective_id=0, has_side_effects=True, vmem_limit_bytes=60 * 1024 * 1024,
        ),
    )(
        span_order,
        queries.reshape(rows * HEADS, DIM),
        out_grad.reshape(rows * HEADS, DIM),
        key_rows.reshape(rows, DIM),
        value_slot_rows.reshape(rows, DIM),
    )
    return (
        dq.reshape(rows, HEADS, DIM),
        dk.reshape(rows, 1, DIM),
        dv.reshape(rows, 1, DIM),
    )


def solution(mesh):
    row = P(("seq", "ctx"), "tp", None)
    return jax.shard_map(
        local,
        mesh=mesh,
        in_specs=(row, row, row, row, P("seq")),
        out_specs=(row, row, row),
        check_vma=False,
    )
```

```python
import math

import jax
import jax.numpy as jnp
from jax import lax
from jax.experimental import pallas as pl
from jax.experimental.pallas import tpu as pltpu
from jax.sharding import PartitionSpec as P

MESH = pl.DeviceIdType.MESH
SPAN = 128
HEADS = 4
DIM = 128
COLS = 2 * HEADS * SPAN
CHUNK = 4 * SPAN
WIDE = 256
TILES = COLS // WIDE
BLOCK = 64
HIDDEN = -1e30
F32 = jnp.float32
BF16 = jnp.bfloat16

CHUNKS = (
    ((0, 0, 0), (1, 0, 0), (0, 1, 0), (0, 3, 0)),
    ((0, 0, 1), (1, 0, 1), (1, 1, 0), (1, 3, 0)),
    ((0, 1, 1), (0, 3, 1), (1, 1, 1), (1, 3, 1)),
    ((0, 2, 0), (1, 2, 0), (0, 2, 1), (1, 2, 1)),
)
FORWARD = (
    (0, 0), (1, 0), (2, 0), (3, 0), (4, 0), (0, 1), (1, 1), (2, 1),
    (3, 1), (5, 0), (4, 1), (5, 1), (6, 0), (7, 0), (6, 1), (7, 1),
)
BACKWARD = (
    (7, 1), (7, 0), (6, 1), (6, 0), (5, 1), (5, 0), (4, 1), (4, 0),
    (3, 1), (3, 0), (2, 1), (2, 0), (1, 1), (0, 1), (1, 0), (0, 0),
)
PLACE = {unit: 4 * i + j for i, units in enumerate(CHUNKS) for j, unit in enumerate(units)}


def pick(step, values):
    return sum(jnp.where(step == i, v, 0) for i, v in enumerate(values) if v)


def when(condition):
    def run(body):
        lax.fori_loop(0, condition.astype(jnp.int32), lambda _, c: (body(), c)[1], 0)

    return run


def kernel(
    span_ref, q_ref, g_ref, k_ref, v_ref,
    dq_ref, dk_ref, dv_ref,
    kv, part, stage, half_in, x_in, e_in, z_in, dq_out, dq_in,
    qt, gt, qrows, grows, lhs, sbuf, pbuf, dsbuf, dqt, top, total, delta, stats_out, stats_in,
    spans, own_spans,
    load_sem, gather_send, gather_recv, gather_z, q_send, q_recv, stat_send, stat_recv,
    reduce_send, reduce_recv, reduce_z, dq_send, dq_recv,
):
    me = lax.axis_index("ctx")
    x, z, y = me // 8, (me // 4) % 2, me % 4

    def at(xx, zz, yy):
        return (xx % 4) * 8 + (zz % 2) * 4 + yy

    x_ways = (at(x + 1, z, y), at(x + 3, z, y))
    partner = at(x, z, y + 1 - 2 * (y % 2))
    other = at(x, z, 3 - y)
    z_other = at(x, z + 1, y)

    def slot_of(base, c, da, e):
        return base + PLACE[(c, da, e)]

    loads = []
    for c in range(2):
        own = slot_of(0, c, 0, 0)
        rows = pl.ds(c * SPAN, SPAN)
        loads.append(pltpu.make_async_copy(k_ref.at[rows], kv.at[own, 0], load_sem.at[2 * c]))
        loads.append(pltpu.make_async_copy(v_ref.at[rows], kv.at[own, 1], load_sem.at[2 * c + 1]))
    loads.append(pltpu.make_async_copy(q_ref, qrows.at[0], load_sem.at[4]))
    loads.append(pltpu.make_async_copy(g_ref, grows.at[0], load_sem.at[5]))
    for copy in loads:
        copy.start()

    barrier = pltpu.get_barrier_semaphore()
    for device in (*x_ways, partner, other, z_other):
        pl.semaphore_signal(barrier, inc=1, device_id={"ctx": device}, device_id_type=MESH)
    pl.semaphore_wait(barrier, 5)
    for copy in loads[:4]:
        copy.wait()

    def send(src, dst, send_sem, recv_sem, device):
        pltpu.make_async_remote_copy(
            src_ref=src, dst_ref=dst, send_sem=send_sem, recv_sem=recv_sem,
            device_id={"ctx": device}, device_id_type=MESH,
        ).start()

    def await_units(sem, units):
        block = kv.at[pl.ds(0, units)]
        pltpu.make_async_copy(block, block, sem).wait()

    def gather(dz, group, src, dst, device):
        send(src, dst, gather_send, gather_recv.at[dz, group], device)

    def arrived(dz, *groups):
        for group in groups:
            await_units(gather_recv.at[dz, group], (1, 2, 1, 2, 1, 1, 2, 1, 2, 1)[group])

    def along_x(dz, group, c, e):
        unit = kv.at[slot_of(16 * dz, c, 0, e)]
        gather(dz, group, unit, kv.at[slot_of(16 * dz, c, 3, e)], x_ways[0])
        gather(dz, group, unit, kv.at[slot_of(16 * dz, c, 1, e)], x_ways[1])

    def opposite_x(dz, group, c, e):
        there, up, down = (slot_of(16 * dz, c, da, e) for da in (2, 3, 1))
        gather(dz, group, kv.at[up, 0], kv.at[there, 0], x_ways[0])
        gather(dz, group, kv.at[down, 1], kv.at[there, 1], x_ways[1])

    def across(dz, group, c, da):
        src, dst = slot_of(16 * dz, c, da, 0), slot_of(16 * dz, c, da, 1)
        gather(dz, group, kv.at[src], kv.at[dst], other)

    def gather_own(dz):
        along_x(dz, 1, 0, 0)
        across(dz, 0, 0, 0)
        along_x(dz, 8, 1, 0)
        across(dz, 5, 1, 0)

    def gather_a(dz):
        arrived(dz, 1)
        opposite_x(dz, 2, 0, 0)
        arrived(dz, 0)
        along_x(dz, 3, 0, 1)

    def gather_b(dz):
        arrived(dz, 8)
        opposite_x(dz, 9, 1, 0)
        across(dz, 6, 1, 1)
        across(dz, 6, 1, 3)

    def gather_c(dz):
        arrived(dz, 9)
        across(dz, 7, 1, 2)
        arrived(dz, 3)
        opposite_x(dz, 4, 0, 1)

    for c in range(2):
        send(
            kv.at[slot_of(0, c, 0, 0)], kv.at[slot_of(16, c, 0, 0)],
            gather_send, gather_z, z_other,
        )
    gather_own(0)
    for copy in loads[4:]:
        copy.wait()
    send(qrows.at[0], qrows.at[1], q_send, q_recv, partner)
    send(grows.at[0], grows.at[1], q_send, q_recv, partner)

    for dz in range(2):
        for c, da, e in PLACE:
            owner = at(x + da, z + dz, y if e == 0 else 3 - y)
            spans[slot_of(16 * dz, c, da, e)] = span_ref[owner * 2 + c]
    for group, device in enumerate((me, partner)):
        for s in range(2):
            own_spans[group * 2 + s] = span_ref[device * 2 + s]

    lane = lax.broadcasted_iota(jnp.int32, (SPAN, SPAN), 1)
    sublane = lax.broadcasted_iota(jnp.int32, (SPAN, SPAN), 0)

    def prepare(group):
        for block in range(COLS // SPAN):
            here = pl.ds(block * SPAN, SPAN)
            qt[group, 0:DIM, here] = qrows[group, here, :].astype(F32).T.astype(BF16)
            gt[group, :, here] = grows[group, here, :].astype(F32).T.astype(BF16)
            row = block % HEADS * (SPAN // HEADS) + lane // HEADS
            qt[group, DIM : 2 * DIM, here] = jnp.where(row == sublane, 1.0, 0.0).astype(BF16)

    prepare(0)
    top[...] = jnp.full_like(top, HIDDEN)
    total[...] = jnp.zeros_like(total)
    delta[...] = jnp.zeros_like(delta)
    dqt[...] = jnp.zeros_like(dqt)

    exponent = math.log2(math.e) / math.sqrt(DIM)
    scaling = 1.0 / math.sqrt(DIM)

    def masked_keys(chunk, keys, group):
        ahead = sublane - lane
        for s in range(2):
            lhs[s, :, 0:DIM] = keys
            for u in range(4):
                limit = (own_spans[group * 2 + s] - spans[chunk * 4 + u]) * SPAN
                lhs[s, u * SPAN : (u + 1) * SPAN, DIM : 2 * DIM] = jnp.where(
                    ahead > limit, HIDDEN, 0.0
                ).astype(BF16)

    def load_chunk(chunk):
        keys = kv[pl.ds(chunk * 4, 4), 0].reshape(CHUNK, DIM)
        values = kv[pl.ds(chunk * 4, 4), 1].reshape(CHUNK, DIM)
        return keys, values

    def fold(values, op):
        return op(values.reshape(values.shape[0] // 8, 8, WIDE), axis=0)

    def partials(group):
        stats_out[group, :, 0:COLS] = top[group]
        stats_out[group, :, COLS : 2 * COLS] = jnp.sum(total[group], axis=0, keepdims=True)
        stats_out[group, :, 2 * COLS :] = jnp.sum(delta[group], axis=0, keepdims=True)
        send(
            stats_out.at[group], stats_in.at[1 - group],
            stat_send.at[group], stat_recv.at[1 - group], partner,
        )

    def combine(group):
        here, there = stats_out.at[group], stats_in.at[group]
        pltpu.make_async_copy(there, there, stat_recv.at[group]).wait()
        first, second, third = (pl.ds(i * COLS, COLS) for i in range(3))
        highest = jnp.maximum(here[:, first], there[:, first])
        a = jnp.exp2((here[:, first] - highest) * exponent)
        b = jnp.exp2((there[:, first] - highest) * exponent)
        weight = here[:, second] * a + there[:, second] * b
        top[group] = highest + jnp.log(weight) * math.sqrt(DIM)
        delta[group, 0:1, :] = (here[:, third] * a + there[:, third] * b) / weight

    def forward(step, _):
        chunk = pick(step, [c for c, _ in FORWARD])
        group = pick(step, [g for _, g in FORWARD])

        @when(step < 4)
        def _():
            @when(step == 0)
            def _():
                gather_a(0)

            @when(step == 1)
            def _():
                gather_b(0)
                arrived(0, 5)

            @when(step == 2)
            def _():
                gather_c(0)
                await_units(gather_z, 2)
                gather_own(1)
                arrived(0, 6)

            @when(step == 3)
            def _():
                arrived(0, 2, 4, 7)

        @when((step >= 4) & (step < 6))
        def _():
            @when(step == 4)
            def _():
                gather_a(1)

            @when(step == 5)
            def _():
                gather_b(1)
                await_units(q_recv, 8)
                prepare(1)

        @when(step >= 8)
        def _():
            @when(step == 8)
            def _():
                gather_c(1)
                arrived(1, 5)

            @when(step == 12)
            def _():
                arrived(1, 6)

            @when(step == 13)
            def _():
                arrived(1, 2, 4, 7)

            @when(step == 14)
            def _():
                partials(0)

        keys, values = load_chunk(chunk)

        def grads(tile):
            cols = pl.ds(tile * WIDE, WIDE)
            return jnp.dot(values, gt[group, :, cols], preferred_element_type=F32)

        def topped(tile):
            cols = pl.ds(tile * WIDE, WIDE)
            s = tile * WIDE // (HEADS * SPAN)
            score = jnp.dot(lhs[s], qt[group, :, cols], preferred_element_type=F32)
            sbuf[chunk * 2 + group, :, cols] = score
            before = top[group, :, cols]
            now = jnp.maximum(before, jnp.max(fold(score, jnp.max), axis=0, keepdims=True))
            top[group, :, cols] = now
            return now, jnp.exp2((before - now) * exponent)

        masked_keys(chunk, keys, group)
        ahead = topped(0)
        for tile in range(TILES):
            cols = pl.ds(tile * WIDE, WIDE)
            now, rescale = ahead
            if tile + 1 < TILES:
                ahead = topped(tile + 1)
            grad_probs = grads(tile)
            weight = total[group, :, cols] * rescale
            product = delta[group, :, cols] * rescale
            for row in range(0, CHUNK, BLOCK):
                score = sbuf[chunk * 2 + group, row : row + BLOCK, cols]
                weights = jnp.exp2((score - now) * exponent)
                weight += fold(weights, jnp.sum)
                product += fold(weights * grad_probs[row : row + BLOCK], jnp.sum)
            total[group, :, cols] = weight
            delta[group, :, cols] = product
        return 0

    lax.fori_loop(0, 16, forward, 0)
    partials(1)
    combine(1)

    def reduce(dz, group, src, dst, device):
        send(src, dst, reduce_send, reduce_recv.at[dz, group], device)

    def put(slot, sums):
        stage[slot, 0] = sums[0].astype(BF16)
        stage[slot, 1] = sums[1].astype(BF16)

    def partial_of(slot):
        return [part[slot, 0], part[slot, 1]]

    def plus(sums, ref):
        return [sums[i] + ref[i].astype(F32) for i in range(2)]

    def plus_half(sums, slot, which):
        arrived = half_in[slot].astype(F32)
        return [sums[0] + arrived, sums[1]] if which == 0 else [sums[0], sums[1] + arrived]

    def halves(base, dz, group, c, e, sums):
        slot = slot_of(base, c, 2, e)
        put(slot, sums)
        reduce(dz, group, stage.at[slot, 0], half_in.at[slot_of(base, c, 1, e)], x_ways[0])
        reduce(dz, group, stage.at[slot, 1], half_in.at[slot_of(base, c, 3, e)], x_ways[1])

    def sum_along_x(base, dz, group, c, e, kind, way, sums):
        slot = slot_of(base, c, (1, 3)[way], e)
        put(slot, plus_half(sums, slot, way))
        reduce(dz, group, stage.at[slot], x_in.at[dz, kind, way], x_ways[way])

    def sum_across(base, dz, group, c, da, place, sums):
        slot = slot_of(base, c, da, 1)
        put(slot, sums)
        reduce(dz, group, stage.at[slot], e_in.at[dz, place], other)

    def landed(dz, *groups):
        for group in groups:
            await_units(reduce_recv.at[dz, group], (1, 1, 2, 2, 1, 2, 2, 1, 1, 1)[group])

    def reduce_d(dz):
        base = 16 * dz
        sum_across(base, dz, 1, 1, 2, 2, partial_of(slot_of(base, 1, 2, 1)))
        halves(base, dz, 0, 0, 1, partial_of(slot_of(base, 0, 2, 1)))
        halves(base, dz, 9, 0, 0, partial_of(slot_of(base, 0, 2, 0)))

    def reduce_c(dz):
        base = 16 * dz
        for da in (1, 3):
            sum_across(base, dz, 3, 1, da, da, partial_of(slot_of(base, 1, da, 1)))
        landed(dz, 0)
        for way, da in enumerate((1, 3)):
            sum_along_x(base, dz, 2, 0, 1, 1, way, partial_of(slot_of(base, 0, da, 1)))

    def reduce_c_opposite(dz):
        base = 16 * dz
        landed(dz, 1)
        halves(base, dz, 4, 1, 0, plus(partial_of(slot_of(base, 1, 2, 0)), e_in.at[dz, 2]))

    def reduce_b(dz):
        base = 16 * dz
        sum_across(base, dz, 8, 1, 0, 0, partial_of(slot_of(base, 1, 0, 1)))
        landed(dz, 2)
        sums = partial_of(slot_of(base, 0, 0, 1))
        for way in range(2):
            sums = plus(sums, x_in.at[dz, 1, way])
        sum_across(base, dz, 7, 0, 0, 4, sums)

    def reduce_b_along(dz):
        base = 16 * dz
        landed(dz, 3, 4)
        for way, da in enumerate((1, 3)):
            sums = plus(partial_of(slot_of(base, 1, da, 0)), e_in.at[dz, da])
            sum_along_x(base, dz, 6, 1, 0, 2, way, sums)

    def reduce_a(dz):
        base = 16 * dz
        landed(dz, 9)
        for way, da in enumerate((1, 3)):
            sum_along_x(base, dz, 5, 0, 0, 0, way, partial_of(slot_of(base, 0, da, 0)))

    def own_sums(dz):
        landed(dz, 7, 8, 6, 5)
        for c in range(2):
            slot = slot_of(16 * dz, c, 0, 0)
            sums = partial_of(slot)
            for way in range(2):
                sums = plus(sums, x_in.at[dz, 2 * c, way])
            yield c, slot, plus(sums, e_in.at[dz, 4 - 4 * c])

    def query_grads(group):
        for block in range(COLS // SPAN):
            here = pl.ds(block * SPAN, SPAN)
            yield here, (dqt[group, :, here] * scaling).T

    def backward(step, _):
        chunk = pick(step, [c for c, _ in BACKWARD])
        group = pick(step, [g for _, g in BACKWARD])

        @pl.when(step == 1)
        def _():
            combine(0)

        keys, values = load_chunk(chunk)
        for tile in range(TILES):
            cols = pl.ds(tile * WIDE, WIDE)
            grad_probs = jnp.dot(values, gt[group, :, cols], preferred_element_type=F32)
            lse, mean = top[group, :, cols], delta[group, 0:1, cols]
            for row in range(0, CHUNK, BLOCK):
                rows = slice(row, row + BLOCK)
                score = sbuf[chunk * 2 + group, rows, cols]
                probs = jnp.exp2((score - lse) * exponent)
                pbuf[rows, cols] = probs.astype(BF16)
                dsbuf[rows, cols] = (probs * (grad_probs[rows] - mean)).astype(BF16)
        units = pl.ds(chunk * 4, 4)
        value_part = jnp.dot(pbuf[...], grows[group], preferred_element_type=F32)
        key_part = jnp.dot(dsbuf[...], qrows[group], preferred_element_type=F32) * scaling
        for which, found in ((1, value_part), (0, key_part)):
            before = jnp.where(group == 1, 0.0, part[units, which])
            part[units, which] = before + found.reshape(4, SPAN, DIM)
        keys_t = keys.astype(F32).T.astype(BF16)
        dqt[group] += jnp.dot(keys_t, dsbuf[...], preferred_element_type=F32)

        events = (
            (1, 9, reduce_d), (3, 11, reduce_c), (4, 12, reduce_c_opposite), (6, 14, reduce_b),
            (7, 14, reduce_b_along),
        )
        for early, late, event in events:

            @pl.when((step == early) | (step == late))
            def _():
                event(jnp.where(step < 8, 1, 0))

        @pl.when(step == 7)
        def _():
            reduce_a(1)

        @pl.when(step == 10)
        def _():
            for c, slot, sums in own_sums(1):
                put(slot, sums)
                send(stage.at[slot], z_in.at[c], reduce_send, reduce_z, z_other)

        @pl.when(step == 13)
        def _():
            for here, block in query_grads(1):
                dq_out[here, :] = block.astype(BF16)
            send(dq_out, dq_in, dq_send, dq_recv, partner)

        return 0

    lax.fori_loop(0, 16, backward, 0)
    reduce_a(0)
    await_units(reduce_z, 2)
    for c, _, sums in own_sums(0):
        rows = pl.ds(c * SPAN, SPAN)
        dk_ref[rows, :] = (sums[0] + z_in[c, 0].astype(F32)).astype(BF16)
        dv_ref[rows, :] = (sums[1] + z_in[c, 1].astype(F32)).astype(BF16)
    await_units(dq_recv, 4)
    for here, block in query_grads(0):
        dq_ref[here, :] = (block + dq_in[here, :].astype(F32)).astype(BF16)
    await_units(gather_send, 30)
    await_units(q_send, 8)
    await_units(reduce_send, 30)
    await_units(dq_send, 4)
    for group in range(2):
        sent = stats_out.at[group]
        pltpu.make_async_copy(sent, sent, stat_send.at[group]).wait()


def settle(*refs):
    count = (len(refs) - 2) // 3
    sources, targets, held = (refs[i * count : (i + 1) * count] for i in range(3))
    in_sem, out_sem = refs[-2:]
    copies = []
    for i, (source, target, buffer) in enumerate(zip(sources, targets, held)):
        copies.append((
            pltpu.make_async_copy(source, buffer, in_sem.at[i]),
            pltpu.make_async_copy(buffer, target, out_sem.at[i]),
        ))
    for inward, _ in copies:
        inward.start()
    for inward, outward in copies:
        inward.wait()
        outward.start()
    for _, outward in copies:
        outward.wait()


def settled(*results):
    anywhere = [pl.BlockSpec(memory_space=pl.ANY)] * len(results)
    return pl.pallas_call(
        settle,
        out_shape=tuple(jax.ShapeDtypeStruct(r.shape, r.dtype) for r in results),
        in_specs=anywhere,
        out_specs=tuple(anywhere),
        scratch_shapes=[
            *(pltpu.VMEM(r.shape, r.dtype) for r in results),
            pltpu.SemaphoreType.DMA((len(results),)),
            pltpu.SemaphoreType.DMA((len(results),)),
        ],
    )(*results)


def local(queries, key_rows, value_slot_rows, out_grad, span_order):
    rows = queries.shape[0]
    vmem = pl.BlockSpec(memory_space=pltpu.VMEM)
    unit = (2, SPAN, DIM)
    dma = pltpu.SemaphoreType.DMA
    dq, dk, dv = pl.pallas_call(
        kernel,
        out_shape=(
            jax.ShapeDtypeStruct((rows * HEADS, DIM), BF16),
            jax.ShapeDtypeStruct((rows, DIM), BF16),
            jax.ShapeDtypeStruct((rows, DIM), BF16),
        ),
        in_specs=[
            pl.BlockSpec(memory_space=pltpu.SMEM),
            *([pl.BlockSpec(memory_space=pl.ANY)] * 4),
        ],
        out_specs=(vmem, vmem, vmem),
        scratch_shapes=[
            pltpu.VMEM((32,) + unit, BF16),
            pltpu.VMEM((32,) + unit, F32),
            pltpu.VMEM((32,) + unit, BF16),
            pltpu.VMEM((32, SPAN, DIM), BF16),
            pltpu.VMEM((2, 3, 2) + unit, BF16),
            pltpu.VMEM((2, 5) + unit, BF16),
            pltpu.VMEM((2,) + unit, BF16),
            pltpu.VMEM((COLS, DIM), BF16),
            pltpu.VMEM((COLS, DIM), BF16),
            pltpu.VMEM((2, 2 * DIM, COLS), BF16),
            pltpu.VMEM((2, DIM, COLS), BF16),
            pltpu.VMEM((2, COLS, DIM), BF16),
            pltpu.VMEM((2, COLS, DIM), BF16),
            pltpu.VMEM((2, CHUNK, 2 * DIM), BF16),
            pltpu.VMEM((16, CHUNK, COLS), F32),
            pltpu.VMEM((CHUNK, COLS), BF16),
            pltpu.VMEM((CHUNK, COLS), BF16),
            pltpu.VMEM((2, DIM, COLS), F32),
            pltpu.VMEM((2, 1, COLS), F32),
            pltpu.VMEM((2, 8, COLS), F32),
            pltpu.VMEM((2, 8, COLS), F32),
            pltpu.VMEM((2, 1, 3 * COLS), F32),
            pltpu.VMEM((2, 1, 3 * COLS), F32),
            pltpu.SMEM((32,), jnp.int32),
            pltpu.SMEM((4,), jnp.int32),
            dma((6,)), dma, dma((2, 10)), dma, dma, dma, dma((2,)), dma((2,)),
            dma, dma((2, 10)), dma, dma, dma,
        ],
        compiler_params=pltpu.CompilerParams(
            collective_id=0, has_side_effects=True, vmem_limit_bytes=60 * 1024 * 1024,
        ),
    )(
        span_order,
        queries.reshape(rows * HEADS, DIM),
        out_grad.reshape(rows * HEADS, DIM),
        key_rows.reshape(rows, DIM),
        value_slot_rows.reshape(rows, DIM),
    )
    dq, dk, dv = settled(dq, dk, dv)
    return (
        dq.reshape(rows, HEADS, DIM),
        dk.reshape(rows, 1, DIM),
        dv.reshape(rows, 1, DIM),
    )


def solution(mesh):
    row = P(("seq", "ctx"), "tp", None)
    return jax.shard_map(
        local,
        mesh=mesh,
        in_specs=(row, row, row, row, P("seq")),
        out_specs=(row, row, row),
        check_vma=False,
    )
```

```python
import math

import jax
import jax.numpy as jnp
from jax import lax
from jax.experimental import pallas as pl
from jax.experimental.pallas import tpu as pltpu
from jax.sharding import PartitionSpec as P

MESH = pl.DeviceIdType.MESH
SPAN = 128
HEADS = 4
DIM = 128
COLS = 2 * HEADS * SPAN
CHUNK = 4 * SPAN
WIDE = 256
TILES = COLS // WIDE
BLOCK = 64
HIDDEN = -1e30
F32 = jnp.float32
BF16 = jnp.bfloat16

CHUNKS = (
    ((0, 0, 0), (1, 0, 0), (0, 1, 0), (0, 3, 0)),
    ((0, 0, 1), (1, 0, 1), (1, 1, 0), (1, 3, 0)),
    ((0, 1, 1), (0, 3, 1), (1, 1, 1), (1, 3, 1)),
    ((0, 2, 0), (1, 2, 0), (0, 2, 1), (1, 2, 1)),
)
FORWARD = (
    (0, 0), (1, 0), (2, 0), (3, 0), (4, 0), (0, 1), (1, 1), (2, 1),
    (3, 1), (5, 0), (4, 1), (5, 1), (6, 0), (7, 0), (6, 1), (7, 1),
)
BACKWARD = (
    (7, 1), (7, 0), (6, 1), (6, 0), (5, 1), (5, 0), (4, 1), (4, 0),
    (3, 1), (3, 0), (2, 1), (2, 0), (1, 1), (0, 1), (1, 0), (0, 0),
)
PLACE = {unit: 4 * i + j for i, units in enumerate(CHUNKS) for j, unit in enumerate(units)}


def pick(step, values):
    return sum(jnp.where(step == i, v, 0) for i, v in enumerate(values) if v)


def when(condition):
    def run(body):
        lax.fori_loop(0, condition.astype(jnp.int32), lambda _, c: (body(), c)[1], 0)

    return run


def kernel(
    span_ref, q_ref, g_ref, k_ref, v_ref,
    dq_ref, dk_ref, dv_ref,
    kv, part, stage, half_in, x_in, e_in, z_in, dq_out, dq_in,
    qt, gt, qrows, grows, masks, sbuf, pbuf, dsbuf, dqt, top, total, delta, stats_out, stats_in,
    spans, own_spans,
    load_sem, gather_send, gather_recv, gather_z, q_send, q_recv, stat_send, stat_recv,
    reduce_send, reduce_recv, reduce_z, dq_send, dq_recv,
):
    me = lax.axis_index("ctx")
    x, z, y = me // 8, (me // 4) % 2, me % 4

    def at(xx, zz, yy):
        return (xx % 4) * 8 + (zz % 2) * 4 + yy

    x_ways = (at(x + 1, z, y), at(x + 3, z, y))
    partner = at(x, z, y + 1 - 2 * (y % 2))
    other = at(x, z, 3 - y)
    z_other = at(x, z + 1, y)

    def slot_of(base, c, da, e):
        return base + PLACE[(c, da, e)]

    loads = []
    for c in range(2):
        own = slot_of(0, c, 0, 0)
        rows = pl.ds(c * SPAN, SPAN)
        loads.append(pltpu.make_async_copy(k_ref.at[rows], kv.at[own, 0], load_sem.at[2 * c]))
        loads.append(pltpu.make_async_copy(v_ref.at[rows], kv.at[own, 1], load_sem.at[2 * c + 1]))
    loads.append(pltpu.make_async_copy(q_ref, qrows.at[0], load_sem.at[4]))
    loads.append(pltpu.make_async_copy(g_ref, grows.at[0], load_sem.at[5]))
    for copy in loads:
        copy.start()

    barrier = pltpu.get_barrier_semaphore()
    for device in (*x_ways, partner, other, z_other):
        pl.semaphore_signal(barrier, inc=1, device_id={"ctx": device}, device_id_type=MESH)
    pl.semaphore_wait(barrier, 5)
    for copy in loads[:4]:
        copy.wait()

    def send(src, dst, send_sem, recv_sem, device):
        pltpu.make_async_remote_copy(
            src_ref=src, dst_ref=dst, send_sem=send_sem, recv_sem=recv_sem,
            device_id={"ctx": device}, device_id_type=MESH,
        ).start()

    def await_units(sem, units):
        block = kv.at[pl.ds(0, units)]
        pltpu.make_async_copy(block, block, sem).wait()

    def gather(dz, group, src, dst, device):
        send(src, dst, gather_send, gather_recv.at[dz, group], device)

    def arrived(dz, *groups):
        for group in groups:
            await_units(gather_recv.at[dz, group], (1, 2, 1, 2, 1, 1, 2, 1, 2, 1)[group])

    def along_x(dz, group, c, e):
        unit = kv.at[slot_of(16 * dz, c, 0, e)]
        gather(dz, group, unit, kv.at[slot_of(16 * dz, c, 3, e)], x_ways[0])
        gather(dz, group, unit, kv.at[slot_of(16 * dz, c, 1, e)], x_ways[1])

    def opposite_x(dz, group, c, e):
        there, up, down = (slot_of(16 * dz, c, da, e) for da in (2, 3, 1))
        gather(dz, group, kv.at[up, 0], kv.at[there, 0], x_ways[0])
        gather(dz, group, kv.at[down, 1], kv.at[there, 1], x_ways[1])

    def across(dz, group, c, da):
        src, dst = slot_of(16 * dz, c, da, 0), slot_of(16 * dz, c, da, 1)
        gather(dz, group, kv.at[src], kv.at[dst], other)

    def gather_own(dz):
        along_x(dz, 1, 0, 0)
        across(dz, 0, 0, 0)
        along_x(dz, 8, 1, 0)
        across(dz, 5, 1, 0)

    def gather_a(dz):
        arrived(dz, 1)
        opposite_x(dz, 2, 0, 0)
        arrived(dz, 0)
        along_x(dz, 3, 0, 1)

    def gather_b(dz):
        arrived(dz, 8)
        opposite_x(dz, 9, 1, 0)
        across(dz, 6, 1, 1)
        across(dz, 6, 1, 3)

    def gather_c(dz):
        arrived(dz, 9)
        across(dz, 7, 1, 2)
        arrived(dz, 3)
        opposite_x(dz, 4, 0, 1)

    for c in range(2):
        send(
            kv.at[slot_of(0, c, 0, 0)], kv.at[slot_of(16, c, 0, 0)],
            gather_send, gather_z, z_other,
        )
    gather_own(0)
    for copy in loads[4:]:
        copy.wait()
    send(qrows.at[0], qrows.at[1], q_send, q_recv, partner)
    send(grows.at[0], grows.at[1], q_send, q_recv, partner)

    for dz in range(2):
        for c, da, e in PLACE:
            owner = at(x + da, z + dz, y if e == 0 else 3 - y)
            spans[slot_of(16 * dz, c, da, e)] = span_ref[owner * 2 + c]
    for group, device in enumerate((me, partner)):
        for s in range(2):
            own_spans[group * 2 + s] = span_ref[device * 2 + s]

    lane = lax.broadcasted_iota(jnp.int32, (SPAN, SPAN), 1)
    sublane = lax.broadcasted_iota(jnp.int32, (SPAN, SPAN), 0)

    def prepare(group):
        for block in range(COLS // SPAN):
            here = pl.ds(block * SPAN, SPAN)
            qt[group, 0:DIM, here] = qrows[group, here, :].astype(F32).T.astype(BF16)
            gt[group, :, here] = grows[group, here, :].astype(F32).T.astype(BF16)
            row = block % HEADS * (SPAN // HEADS) + lane // HEADS
            qt[group, DIM : 2 * DIM, here] = jnp.where(row == sublane, 1.0, 0.0).astype(BF16)

    prepare(0)
    top[...] = jnp.full_like(top, HIDDEN)
    total[...] = jnp.zeros_like(total)
    delta[...] = jnp.zeros_like(delta)
    dqt[...] = jnp.zeros_like(dqt)

    exponent = math.log2(math.e) / math.sqrt(DIM)
    scaling = 1.0 / math.sqrt(DIM)

    def mask_step(place, _):
        chunk, group = place // 2, place % 2
        ahead = sublane - lane
        for s in range(2):
            for u in range(4):
                limit = (own_spans[group * 2 + s] - spans[chunk * 4 + u]) * SPAN
                masks[place, s, u * SPAN : (u + 1) * SPAN, :] = jnp.where(
                    ahead > limit, HIDDEN, 0.0
                ).astype(BF16)
        return 0

    lax.fori_loop(0, 16, mask_step, 0)

    def load_chunk(chunk):
        keys = kv[pl.ds(chunk * 4, 4), 0].reshape(CHUNK, DIM)
        values = kv[pl.ds(chunk * 4, 4), 1].reshape(CHUNK, DIM)
        return keys, values

    def fold(values, op):
        return op(values.reshape(values.shape[0] // 8, 8, WIDE), axis=0)

    def partials(group):
        stats_out[group, :, 0:COLS] = top[group]
        stats_out[group, :, COLS : 2 * COLS] = jnp.sum(total[group], axis=0, keepdims=True)
        stats_out[group, :, 2 * COLS :] = jnp.sum(delta[group], axis=0, keepdims=True)
        send(
            stats_out.at[group], stats_in.at[1 - group],
            stat_send.at[group], stat_recv.at[1 - group], partner,
        )

    def combine(group):
        here, there = stats_out.at[group], stats_in.at[group]
        pltpu.make_async_copy(there, there, stat_recv.at[group]).wait()
        first, second, third = (pl.ds(i * COLS, COLS) for i in range(3))
        highest = jnp.maximum(here[:, first], there[:, first])
        a = jnp.exp2((here[:, first] - highest) * exponent)
        b = jnp.exp2((there[:, first] - highest) * exponent)
        weight = here[:, second] * a + there[:, second] * b
        top[group] = highest + jnp.log(weight) * math.sqrt(DIM)
        delta[group, 0:1, :] = (here[:, third] * a + there[:, third] * b) / weight

    def forward(step, _):
        chunk = pick(step, [c for c, _ in FORWARD])
        group = pick(step, [g for _, g in FORWARD])

        @when(step < 4)
        def _():
            @when(step == 0)
            def _():
                gather_a(0)

            @when(step == 1)
            def _():
                gather_b(0)
                arrived(0, 5)

            @when(step == 2)
            def _():
                gather_c(0)
                await_units(gather_z, 2)
                gather_own(1)
                arrived(0, 6)

            @when(step == 3)
            def _():
                arrived(0, 2, 4, 7)

        @when((step >= 4) & (step < 6))
        def _():
            @when(step == 4)
            def _():
                gather_a(1)

            @when(step == 5)
            def _():
                gather_b(1)
                await_units(q_recv, 8)
                prepare(1)

        @when(step >= 8)
        def _():
            @when(step == 8)
            def _():
                gather_c(1)
                arrived(1, 5)

            @when(step == 12)
            def _():
                arrived(1, 6)

            @when(step == 13)
            def _():
                arrived(1, 2, 4, 7)

            @when(step == 14)
            def _():
                partials(0)

        keys, values = load_chunk(chunk)

        def grads(tile):
            cols = pl.ds(tile * WIDE, WIDE)
            return jnp.dot(values, gt[group, :, cols], preferred_element_type=F32)

        def topped(tile):
            cols = pl.ds(tile * WIDE, WIDE)
            s = tile * WIDE // (HEADS * SPAN)
            place = chunk * 2 + group
            masked = jnp.concatenate([keys, masks[place, s]], axis=1)
            score = jnp.dot(masked, qt[group, :, cols], preferred_element_type=F32)
            sbuf[place, :, cols] = score
            before = top[group, :, cols]
            now = jnp.maximum(before, jnp.max(fold(score, jnp.max), axis=0, keepdims=True))
            top[group, :, cols] = now
            return now, jnp.exp2((before - now) * exponent)

        ahead = topped(0)
        for tile in range(TILES):
            cols = pl.ds(tile * WIDE, WIDE)
            now, rescale = ahead
            if tile + 1 < TILES:
                ahead = topped(tile + 1)
            grad_probs = grads(tile)
            weight = total[group, :, cols] * rescale
            product = delta[group, :, cols] * rescale
            for row in range(0, CHUNK, BLOCK):
                score = sbuf[chunk * 2 + group, row : row + BLOCK, cols]
                weights = jnp.exp2((score - now) * exponent)
                weight += fold(weights, jnp.sum)
                product += fold(weights * grad_probs[row : row + BLOCK], jnp.sum)
            total[group, :, cols] = weight
            delta[group, :, cols] = product
        return 0

    lax.fori_loop(0, 16, forward, 0)
    partials(1)
    combine(1)

    def reduce(dz, group, src, dst, device):
        send(src, dst, reduce_send, reduce_recv.at[dz, group], device)

    def put(slot, sums):
        stage[slot, 0] = sums[0].astype(BF16)
        stage[slot, 1] = sums[1].astype(BF16)

    def partial_of(slot):
        return [part[slot, 0], part[slot, 1]]

    def plus(sums, ref):
        return [sums[i] + ref[i].astype(F32) for i in range(2)]

    def plus_half(sums, slot, which):
        arrived = half_in[slot].astype(F32)
        return [sums[0] + arrived, sums[1]] if which == 0 else [sums[0], sums[1] + arrived]

    def halves(base, dz, group, c, e, sums):
        slot = slot_of(base, c, 2, e)
        put(slot, sums)
        reduce(dz, group, stage.at[slot, 0], half_in.at[slot_of(base, c, 1, e)], x_ways[0])
        reduce(dz, group, stage.at[slot, 1], half_in.at[slot_of(base, c, 3, e)], x_ways[1])

    def sum_along_x(base, dz, group, c, e, kind, way, sums):
        slot = slot_of(base, c, (1, 3)[way], e)
        put(slot, plus_half(sums, slot, way))
        reduce(dz, group, stage.at[slot], x_in.at[dz, kind, way], x_ways[way])

    def sum_across(base, dz, group, c, da, place, sums):
        slot = slot_of(base, c, da, 1)
        put(slot, sums)
        reduce(dz, group, stage.at[slot], e_in.at[dz, place], other)

    def landed(dz, *groups):
        for group in groups:
            await_units(reduce_recv.at[dz, group], (1, 1, 2, 2, 1, 2, 2, 1, 1, 1)[group])

    def reduce_d(dz):
        base = 16 * dz
        sum_across(base, dz, 1, 1, 2, 2, partial_of(slot_of(base, 1, 2, 1)))
        halves(base, dz, 0, 0, 1, partial_of(slot_of(base, 0, 2, 1)))
        halves(base, dz, 9, 0, 0, partial_of(slot_of(base, 0, 2, 0)))

    def reduce_c(dz):
        base = 16 * dz
        for da in (1, 3):
            sum_across(base, dz, 3, 1, da, da, partial_of(slot_of(base, 1, da, 1)))
        landed(dz, 0)
        for way, da in enumerate((1, 3)):
            sum_along_x(base, dz, 2, 0, 1, 1, way, partial_of(slot_of(base, 0, da, 1)))

    def reduce_c_opposite(dz):
        base = 16 * dz
        landed(dz, 1)
        halves(base, dz, 4, 1, 0, plus(partial_of(slot_of(base, 1, 2, 0)), e_in.at[dz, 2]))

    def reduce_b(dz):
        base = 16 * dz
        sum_across(base, dz, 8, 1, 0, 0, partial_of(slot_of(base, 1, 0, 1)))
        landed(dz, 2)
        sums = partial_of(slot_of(base, 0, 0, 1))
        for way in range(2):
            sums = plus(sums, x_in.at[dz, 1, way])
        sum_across(base, dz, 7, 0, 0, 4, sums)

    def reduce_b_along(dz):
        base = 16 * dz
        landed(dz, 3, 4)
        for way, da in enumerate((1, 3)):
            sums = plus(partial_of(slot_of(base, 1, da, 0)), e_in.at[dz, da])
            sum_along_x(base, dz, 6, 1, 0, 2, way, sums)

    def reduce_a(dz):
        base = 16 * dz
        landed(dz, 9)
        for way, da in enumerate((1, 3)):
            sum_along_x(base, dz, 5, 0, 0, 0, way, partial_of(slot_of(base, 0, da, 0)))

    def own_sums(dz):
        landed(dz, 7, 8, 6, 5)
        for c in range(2):
            slot = slot_of(16 * dz, c, 0, 0)
            sums = partial_of(slot)
            for way in range(2):
                sums = plus(sums, x_in.at[dz, 2 * c, way])
            yield c, slot, plus(sums, e_in.at[dz, 4 - 4 * c])

    def query_grads(group):
        for block in range(COLS // SPAN):
            here = pl.ds(block * SPAN, SPAN)
            yield here, (dqt[group, :, here] * scaling).T

    def backward(step, _):
        chunk = pick(step, [c for c, _ in BACKWARD])
        group = pick(step, [g for _, g in BACKWARD])

        @pl.when(step == 1)
        def _():
            combine(0)

        keys, values = load_chunk(chunk)
        for tile in range(TILES):
            cols = pl.ds(tile * WIDE, WIDE)
            grad_probs = jnp.dot(values, gt[group, :, cols], preferred_element_type=F32)
            lse, mean = top[group, :, cols], delta[group, 0:1, cols]
            for row in range(0, CHUNK, BLOCK):
                rows = slice(row, row + BLOCK)
                score = sbuf[chunk * 2 + group, rows, cols]
                probs = jnp.exp2((score - lse) * exponent)
                pbuf[rows, cols] = probs.astype(BF16)
                dsbuf[rows, cols] = (probs * (grad_probs[rows] - mean)).astype(BF16)
        units = pl.ds(chunk * 4, 4)
        value_part = jnp.dot(pbuf[...], grows[group], preferred_element_type=F32)
        key_part = jnp.dot(dsbuf[...], qrows[group], preferred_element_type=F32) * scaling
        for which, found in ((1, value_part), (0, key_part)):
            before = jnp.where(group == 1, 0.0, part[units, which])
            part[units, which] = before + found.reshape(4, SPAN, DIM)
        keys_t = keys.astype(F32).T.astype(BF16)
        dqt[group] += jnp.dot(keys_t, dsbuf[...], preferred_element_type=F32)

        events = (
            (1, 9, reduce_d), (3, 11, reduce_c), (4, 12, reduce_c_opposite), (6, 14, reduce_b),
            (7, 14, reduce_b_along),
        )
        for early, late, event in events:

            @pl.when((step == early) | (step == late))
            def _():
                event(jnp.where(step < 8, 1, 0))

        @pl.when(step == 7)
        def _():
            reduce_a(1)

        @pl.when(step == 10)
        def _():
            for c, slot, sums in own_sums(1):
                put(slot, sums)
                send(stage.at[slot], z_in.at[c], reduce_send, reduce_z, z_other)

        @pl.when(step == 13)
        def _():
            for here, block in query_grads(1):
                dq_out[here, :] = block.astype(BF16)
            send(dq_out, dq_in, dq_send, dq_recv, partner)

        return 0

    lax.fori_loop(0, 16, backward, 0)
    reduce_a(0)
    await_units(reduce_z, 2)
    for c, _, sums in own_sums(0):
        rows = pl.ds(c * SPAN, SPAN)
        dk_ref[rows, :] = (sums[0] + z_in[c, 0].astype(F32)).astype(BF16)
        dv_ref[rows, :] = (sums[1] + z_in[c, 1].astype(F32)).astype(BF16)
    await_units(dq_recv, 4)
    for here, block in query_grads(0):
        dq_ref[here, :] = (block + dq_in[here, :].astype(F32)).astype(BF16)
    await_units(gather_send, 30)
    await_units(q_send, 8)
    await_units(reduce_send, 30)
    await_units(dq_send, 4)
    for group in range(2):
        sent = stats_out.at[group]
        pltpu.make_async_copy(sent, sent, stat_send.at[group]).wait()


def settle(*refs):
    count = (len(refs) - 2) // 3
    sources, targets, held = (refs[i * count : (i + 1) * count] for i in range(3))
    in_sem, out_sem = refs[-2:]
    copies = []
    for i, (source, target, buffer) in enumerate(zip(sources, targets, held)):
        copies.append((
            pltpu.make_async_copy(source, buffer, in_sem.at[i]),
            pltpu.make_async_copy(buffer, target, out_sem.at[i]),
        ))
    for inward, _ in copies:
        inward.start()
    for inward, outward in copies:
        inward.wait()
        outward.start()
    for _, outward in copies:
        outward.wait()


def settled(*results):
    anywhere = [pl.BlockSpec(memory_space=pl.ANY)] * len(results)
    return pl.pallas_call(
        settle,
        out_shape=tuple(jax.ShapeDtypeStruct(r.shape, r.dtype) for r in results),
        in_specs=anywhere,
        out_specs=tuple(anywhere),
        scratch_shapes=[
            *(pltpu.VMEM(r.shape, r.dtype) for r in results),
            pltpu.SemaphoreType.DMA((len(results),)),
            pltpu.SemaphoreType.DMA((len(results),)),
        ],
    )(*results)


def local(queries, key_rows, value_slot_rows, out_grad, span_order):
    rows = queries.shape[0]
    vmem = pl.BlockSpec(memory_space=pltpu.VMEM)
    unit = (2, SPAN, DIM)
    dma = pltpu.SemaphoreType.DMA
    dq, dk, dv = pl.pallas_call(
        kernel,
        out_shape=(
            jax.ShapeDtypeStruct((rows * HEADS, DIM), BF16),
            jax.ShapeDtypeStruct((rows, DIM), BF16),
            jax.ShapeDtypeStruct((rows, DIM), BF16),
        ),
        in_specs=[
            pl.BlockSpec(memory_space=pltpu.SMEM),
            *([pl.BlockSpec(memory_space=pl.ANY)] * 4),
        ],
        out_specs=(vmem, vmem, vmem),
        scratch_shapes=[
            pltpu.VMEM((32,) + unit, BF16),
            pltpu.VMEM((32,) + unit, F32),
            pltpu.VMEM((32,) + unit, BF16),
            pltpu.VMEM((32, SPAN, DIM), BF16),
            pltpu.VMEM((2, 3, 2) + unit, BF16),
            pltpu.VMEM((2, 5) + unit, BF16),
            pltpu.VMEM((2,) + unit, BF16),
            pltpu.VMEM((COLS, DIM), BF16),
            pltpu.VMEM((COLS, DIM), BF16),
            pltpu.VMEM((2, 2 * DIM, COLS), BF16),
            pltpu.VMEM((2, DIM, COLS), BF16),
            pltpu.VMEM((2, COLS, DIM), BF16),
            pltpu.VMEM((2, COLS, DIM), BF16),
            pltpu.VMEM((16, 2, CHUNK, SPAN), BF16),
            pltpu.VMEM((16, CHUNK, COLS), F32),
            pltpu.VMEM((CHUNK, COLS), BF16),
            pltpu.VMEM((CHUNK, COLS), BF16),
            pltpu.VMEM((2, DIM, COLS), F32),
            pltpu.VMEM((2, 1, COLS), F32),
            pltpu.VMEM((2, 8, COLS), F32),
            pltpu.VMEM((2, 8, COLS), F32),
            pltpu.VMEM((2, 1, 3 * COLS), F32),
            pltpu.VMEM((2, 1, 3 * COLS), F32),
            pltpu.SMEM((32,), jnp.int32),
            pltpu.SMEM((4,), jnp.int32),
            dma((6,)), dma, dma((2, 10)), dma, dma, dma, dma((2,)), dma((2,)),
            dma, dma((2, 10)), dma, dma, dma,
        ],
        compiler_params=pltpu.CompilerParams(
            collective_id=0, has_side_effects=True, vmem_limit_bytes=60 * 1024 * 1024,
        ),
    )(
        span_order,
        queries.reshape(rows * HEADS, DIM),
        out_grad.reshape(rows * HEADS, DIM),
        key_rows.reshape(rows, DIM),
        value_slot_rows.reshape(rows, DIM),
    )
    dq, dk, dv = settled(dq, dk, dv)
    return (
        dq.reshape(rows, HEADS, DIM),
        dk.reshape(rows, 1, DIM),
        dv.reshape(rows, 1, DIM),
    )


def solution(mesh):
    row = P(("seq", "ctx"), "tp", None)
    return jax.shard_map(
        local,
        mesh=mesh,
        in_specs=(row, row, row, row, P("seq")),
        out_specs=(row, row, row),
        check_vma=False,
    )
```

```python
import math

import jax
import jax.numpy as jnp
from jax import lax
from jax.experimental import pallas as pl
from jax.experimental.pallas import tpu as pltpu
from jax.sharding import PartitionSpec as P

MESH = pl.DeviceIdType.MESH
SPAN = 128
HEADS = 4
DIM = 128
COLS = 2 * HEADS * SPAN
CHUNK = 4 * SPAN
WIDE = 256
TILES = COLS // WIDE
BLOCK = 64
HIDDEN = -1e30
F32 = jnp.float32
BF16 = jnp.bfloat16

CHUNKS = (
    ((0, 0, 0), (1, 0, 0), (0, 1, 0), (0, 3, 0)),
    ((0, 0, 1), (1, 0, 1), (1, 1, 0), (1, 3, 0)),
    ((0, 1, 1), (0, 3, 1), (1, 1, 1), (1, 3, 1)),
    ((0, 2, 0), (1, 2, 0), (0, 2, 1), (1, 2, 1)),
)
FORWARD = (
    (0, 0), (1, 0), (2, 0), (3, 0), (4, 0), (0, 1), (1, 1), (2, 1),
    (3, 1), (5, 0), (4, 1), (5, 1), (6, 0), (7, 0), (6, 1), (7, 1),
)
BACKWARD = (
    (7, 1), (7, 0), (6, 1), (6, 0), (5, 1), (5, 0), (4, 1), (4, 0),
    (3, 1), (3, 0), (2, 1), (2, 0), (1, 1), (0, 1), (1, 0), (0, 0),
)
PLACE = {unit: 4 * i + j for i, units in enumerate(CHUNKS) for j, unit in enumerate(units)}


def pick(step, values):
    return sum(jnp.where(step == i, v, 0) for i, v in enumerate(values) if v)


def when(condition):
    def run(body):
        lax.fori_loop(0, condition.astype(jnp.int32), lambda _, c: (body(), c)[1], 0)

    return run


def kernel(
    span_ref, q_ref, g_ref, k_ref, v_ref,
    dq_ref, dk_ref, dv_ref,
    kv, part, stage, half_in, x_in, e_in, z_in, dq_out, dq_in,
    qt, gt, qrows, grows, masks, sbuf, pbuf, dsbuf, dqt, top, total, delta, stats_out, stats_in,
    spans, own_spans,
    load_sem, gather_send, gather_recv, gather_z, q_send, q_recv, stat_send, stat_recv,
    reduce_send, reduce_recv, reduce_z, dq_send, dq_recv,
):
    me = lax.axis_index("ctx")
    x, z, y = me // 8, (me // 4) % 2, me % 4

    def at(xx, zz, yy):
        return (xx % 4) * 8 + (zz % 2) * 4 + yy

    x_ways = (at(x + 1, z, y), at(x + 3, z, y))
    partner = at(x, z, y + 1 - 2 * (y % 2))
    other = at(x, z, 3 - y)
    z_other = at(x, z + 1, y)

    def slot_of(base, c, da, e):
        return base + PLACE[(c, da, e)]

    loads = []
    for c in range(2):
        own = slot_of(0, c, 0, 0)
        rows = pl.ds(c * SPAN, SPAN)
        loads.append(pltpu.make_async_copy(k_ref.at[rows], kv.at[own, 0], load_sem.at[2 * c]))
        loads.append(pltpu.make_async_copy(v_ref.at[rows], kv.at[own, 1], load_sem.at[2 * c + 1]))
    loads.append(pltpu.make_async_copy(q_ref, qrows.at[0], load_sem.at[4]))
    loads.append(pltpu.make_async_copy(g_ref, grows.at[0], load_sem.at[5]))
    for copy in loads:
        copy.start()

    barrier = pltpu.get_barrier_semaphore()
    for device in (*x_ways, partner, other, z_other):
        pl.semaphore_signal(barrier, inc=1, device_id={"ctx": device}, device_id_type=MESH)
    pl.semaphore_wait(barrier, 5)
    for copy in loads[:4]:
        copy.wait()

    def send(src, dst, send_sem, recv_sem, device):
        pltpu.make_async_remote_copy(
            src_ref=src, dst_ref=dst, send_sem=send_sem, recv_sem=recv_sem,
            device_id={"ctx": device}, device_id_type=MESH,
        ).start()

    def await_units(sem, units):
        block = kv.at[pl.ds(0, units)]
        pltpu.make_async_copy(block, block, sem).wait()

    def gather(dz, group, src, dst, device):
        send(src, dst, gather_send, gather_recv.at[dz, group], device)

    def arrived(dz, *groups):
        for group in groups:
            await_units(gather_recv.at[dz, group], (1, 2, 1, 2, 1, 1, 2, 1, 2, 1)[group])

    def along_x(dz, group, c, e):
        unit = kv.at[slot_of(16 * dz, c, 0, e)]
        gather(dz, group, unit, kv.at[slot_of(16 * dz, c, 3, e)], x_ways[0])
        gather(dz, group, unit, kv.at[slot_of(16 * dz, c, 1, e)], x_ways[1])

    def opposite_x(dz, group, c, e):
        there, up, down = (slot_of(16 * dz, c, da, e) for da in (2, 3, 1))
        gather(dz, group, kv.at[up, 0], kv.at[there, 0], x_ways[0])
        gather(dz, group, kv.at[down, 1], kv.at[there, 1], x_ways[1])

    def across(dz, group, c, da):
        src, dst = slot_of(16 * dz, c, da, 0), slot_of(16 * dz, c, da, 1)
        gather(dz, group, kv.at[src], kv.at[dst], other)

    def gather_own(dz):
        along_x(dz, 1, 0, 0)
        across(dz, 0, 0, 0)
        along_x(dz, 8, 1, 0)
        across(dz, 5, 1, 0)

    def gather_a(dz):
        arrived(dz, 1)
        opposite_x(dz, 2, 0, 0)
        arrived(dz, 0)
        along_x(dz, 3, 0, 1)

    def gather_b(dz):
        arrived(dz, 8)
        opposite_x(dz, 9, 1, 0)
        across(dz, 6, 1, 1)
        across(dz, 6, 1, 3)

    def gather_c(dz):
        arrived(dz, 9)
        across(dz, 7, 1, 2)
        arrived(dz, 3)
        opposite_x(dz, 4, 0, 1)

    for c in range(2):
        send(
            kv.at[slot_of(0, c, 0, 0)], kv.at[slot_of(16, c, 0, 0)],
            gather_send, gather_z, z_other,
        )
    gather_own(0)
    for copy in loads[4:]:
        copy.wait()
    send(qrows.at[0], qrows.at[1], q_send, q_recv, partner)
    send(grows.at[0], grows.at[1], q_send, q_recv, partner)

    for dz in range(2):
        for c, da, e in PLACE:
            owner = at(x + da, z + dz, y if e == 0 else 3 - y)
            spans[slot_of(16 * dz, c, da, e)] = span_ref[owner * 2 + c]
    for group, device in enumerate((me, partner)):
        for s in range(2):
            own_spans[group * 2 + s] = span_ref[device * 2 + s]

    lane = lax.broadcasted_iota(jnp.int32, (SPAN, SPAN), 1)
    sublane = lax.broadcasted_iota(jnp.int32, (SPAN, SPAN), 0)

    def prepare(group):
        for block in range(COLS // SPAN):
            here = pl.ds(block * SPAN, SPAN)
            qt[group, 0:DIM, here] = qrows[group, here, :].astype(F32).T.astype(BF16)
            gt[group, :, here] = grows[group, here, :].astype(F32).T.astype(BF16)
            row = block % HEADS * (SPAN // HEADS) + lane // HEADS
            qt[group, DIM : 2 * DIM, here] = jnp.where(row == sublane, 1.0, 0.0).astype(BF16)

    prepare(0)
    top[...] = jnp.full_like(top, HIDDEN)
    total[...] = jnp.zeros_like(total)
    delta[...] = jnp.zeros_like(delta)
    dqt[...] = jnp.zeros_like(dqt)

    exponent = math.log2(math.e) / math.sqrt(DIM)
    scaling = 1.0 / math.sqrt(DIM)

    def mask_step(place, _):
        chunk, group = place // 2, place % 2
        ahead = sublane - lane
        for s in range(2):
            for u in range(4):
                limit = (own_spans[group * 2 + s] - spans[chunk * 4 + u]) * SPAN
                masks[place, s, u * SPAN : (u + 1) * SPAN, :] = jnp.where(
                    ahead > limit, HIDDEN, 0.0
                ).astype(BF16)
        return 0

    lax.fori_loop(0, 16, mask_step, 0)

    def load_chunk(chunk):
        keys = kv[pl.ds(chunk * 4, 4), 0].reshape(CHUNK, DIM)
        values = kv[pl.ds(chunk * 4, 4), 1].reshape(CHUNK, DIM)
        return keys, values

    def fold(values, op):
        return op(values.reshape(values.shape[0] // 8, 8, WIDE), axis=0)

    def partials(group):
        stats_out[group, :, 0:COLS] = top[group]
        stats_out[group, :, COLS : 2 * COLS] = jnp.sum(total[group], axis=0, keepdims=True)
        stats_out[group, :, 2 * COLS :] = jnp.sum(delta[group], axis=0, keepdims=True)
        send(
            stats_out.at[group], stats_in.at[1 - group],
            stat_send.at[group], stat_recv.at[1 - group], partner,
        )

    def combine(group):
        here, there = stats_out.at[group], stats_in.at[group]
        pltpu.make_async_copy(there, there, stat_recv.at[group]).wait()
        first, second, third = (pl.ds(i * COLS, COLS) for i in range(3))
        highest = jnp.maximum(here[:, first], there[:, first])
        a = jnp.exp2((here[:, first] - highest) * exponent)
        b = jnp.exp2((there[:, first] - highest) * exponent)
        weight = here[:, second] * a + there[:, second] * b
        top[group] = highest + jnp.log(weight) * math.sqrt(DIM)
        delta[group, 0:1, :] = (here[:, third] * a + there[:, third] * b) / weight

    def forward(step, _):
        chunk = pick(step, [c for c, _ in FORWARD])
        group = pick(step, [g for _, g in FORWARD])

        @when(step < 4)
        def _():
            @when(step == 0)
            def _():
                gather_a(0)

            @when(step == 1)
            def _():
                gather_b(0)
                arrived(0, 5)

            @when(step == 2)
            def _():
                gather_c(0)
                await_units(gather_z, 2)
                gather_own(1)
                arrived(0, 6)

            @when(step == 3)
            def _():
                arrived(0, 2, 4, 7)

        @when((step >= 4) & (step < 6))
        def _():
            @when(step == 4)
            def _():
                gather_a(1)

            @when(step == 5)
            def _():
                gather_b(1)
                await_units(q_recv, 8)
                prepare(1)

        @when(step >= 8)
        def _():
            @when(step == 8)
            def _():
                gather_c(1)
                arrived(1, 5)

            @when(step == 12)
            def _():
                arrived(1, 6)

            @when(step == 13)
            def _():
                arrived(1, 2, 4, 7)

            @when(step == 14)
            def _():
                partials(0)

        keys, values = load_chunk(chunk)

        def grads(tile):
            cols = pl.ds(tile * WIDE, WIDE)
            return jnp.dot(values, gt[group, :, cols], preferred_element_type=F32)

        def topped(tile):
            cols = pl.ds(tile * WIDE, WIDE)
            s = tile * WIDE // (HEADS * SPAN)
            place = chunk * 2 + group
            masked = jnp.concatenate([keys, masks[place, s]], axis=1)
            score = jnp.dot(masked, qt[group, :, cols], preferred_element_type=F32)
            sbuf[place, :, cols] = score
            before = top[group, :, cols]
            now = jnp.maximum(before, jnp.max(fold(score, jnp.max), axis=0, keepdims=True))
            top[group, :, cols] = now
            return now, jnp.exp2((before - now) * exponent)

        ahead = topped(0)
        for tile in range(TILES):
            cols = pl.ds(tile * WIDE, WIDE)
            now, rescale = ahead
            if tile + 1 < TILES:
                ahead = topped(tile + 1)
            grad_probs = grads(tile)
            weight = total[group, :, cols] * rescale
            product = delta[group, :, cols] * rescale
            for row in range(0, CHUNK, BLOCK):
                score = sbuf[chunk * 2 + group, row : row + BLOCK, cols]
                weights = jnp.exp2((score - now) * exponent)
                weight += fold(weights, jnp.sum)
                product += fold(weights * grad_probs[row : row + BLOCK], jnp.sum)
            total[group, :, cols] = weight
            delta[group, :, cols] = product
        return 0

    lax.fori_loop(0, 16, forward, 0)
    partials(1)
    combine(1)

    def reduce(dz, group, src, dst, device):
        send(src, dst, reduce_send, reduce_recv.at[dz, group], device)

    def put(slot, sums):
        stage[slot, 0] = sums[0].astype(BF16)
        stage[slot, 1] = sums[1].astype(BF16)

    def partial_of(slot):
        return [part[slot, 0], part[slot, 1]]

    def plus(sums, ref):
        return [sums[i] + ref[i].astype(F32) for i in range(2)]

    def plus_half(sums, slot, which):
        arrived = half_in[slot].astype(F32)
        return [sums[0] + arrived, sums[1]] if which == 0 else [sums[0], sums[1] + arrived]

    def halves(base, dz, group, c, e, sums):
        slot = slot_of(base, c, 2, e)
        put(slot, sums)
        reduce(dz, group, stage.at[slot, 0], half_in.at[slot_of(base, c, 1, e)], x_ways[0])
        reduce(dz, group, stage.at[slot, 1], half_in.at[slot_of(base, c, 3, e)], x_ways[1])

    def sum_along_x(base, dz, group, c, e, kind, way, sums):
        slot = slot_of(base, c, (1, 3)[way], e)
        put(slot, plus_half(sums, slot, way))
        reduce(dz, group, stage.at[slot], x_in.at[dz, kind, way], x_ways[way])

    def sum_across(base, dz, group, c, da, place, sums):
        slot = slot_of(base, c, da, 1)
        put(slot, sums)
        reduce(dz, group, stage.at[slot], e_in.at[dz, place], other)

    def landed(dz, *groups):
        for group in groups:
            await_units(reduce_recv.at[dz, group], (1, 1, 2, 2, 1, 2, 2, 1, 1, 1)[group])

    def reduce_d(dz):
        base = 16 * dz
        sum_across(base, dz, 1, 1, 2, 2, partial_of(slot_of(base, 1, 2, 1)))
        halves(base, dz, 0, 0, 1, partial_of(slot_of(base, 0, 2, 1)))
        halves(base, dz, 9, 0, 0, partial_of(slot_of(base, 0, 2, 0)))

    def reduce_c(dz):
        base = 16 * dz
        for da in (1, 3):
            sum_across(base, dz, 3, 1, da, da, partial_of(slot_of(base, 1, da, 1)))
        landed(dz, 0)
        for way, da in enumerate((1, 3)):
            sum_along_x(base, dz, 2, 0, 1, 1, way, partial_of(slot_of(base, 0, da, 1)))

    def reduce_c_opposite(dz):
        base = 16 * dz
        landed(dz, 1)
        halves(base, dz, 4, 1, 0, plus(partial_of(slot_of(base, 1, 2, 0)), e_in.at[dz, 2]))

    def reduce_b(dz):
        base = 16 * dz
        sum_across(base, dz, 8, 1, 0, 0, partial_of(slot_of(base, 1, 0, 1)))
        landed(dz, 2)
        sums = partial_of(slot_of(base, 0, 0, 1))
        for way in range(2):
            sums = plus(sums, x_in.at[dz, 1, way])
        sum_across(base, dz, 7, 0, 0, 4, sums)

    def reduce_b_along(dz):
        base = 16 * dz
        landed(dz, 3, 4)
        for way, da in enumerate((1, 3)):
            sums = plus(partial_of(slot_of(base, 1, da, 0)), e_in.at[dz, da])
            sum_along_x(base, dz, 6, 1, 0, 2, way, sums)

    def reduce_a(dz):
        base = 16 * dz
        landed(dz, 9)
        for way, da in enumerate((1, 3)):
            sum_along_x(base, dz, 5, 0, 0, 0, way, partial_of(slot_of(base, 0, da, 0)))

    def own_sums(dz):
        landed(dz, 7, 8, 6, 5)
        for c in range(2):
            slot = slot_of(16 * dz, c, 0, 0)
            sums = partial_of(slot)
            for way in range(2):
                sums = plus(sums, x_in.at[dz, 2 * c, way])
            yield c, slot, plus(sums, e_in.at[dz, 4 - 4 * c])

    def query_grads(group):
        for block in range(COLS // SPAN):
            here = pl.ds(block * SPAN, SPAN)
            yield here, (dqt[group, :, here] * scaling).T

    def backward(step, _):
        chunk = pick(step, [c for c, _ in BACKWARD])
        group = pick(step, [g for _, g in BACKWARD])

        @pl.when(step == 1)
        def _():
            combine(0)

        keys, values = load_chunk(chunk)
        for tile in range(TILES):
            cols = pl.ds(tile * WIDE, WIDE)
            grad_probs = jnp.dot(values, gt[group, :, cols], preferred_element_type=F32)
            lse, mean = top[group, :, cols], delta[group, 0:1, cols]
            for row in range(0, CHUNK, BLOCK):
                rows = slice(row, row + BLOCK)
                score = sbuf[chunk * 2 + group, rows, cols]
                probs = jnp.exp2((score - lse) * exponent)
                pbuf[rows, cols] = probs.astype(BF16)
                dsbuf[rows, cols] = (probs * (grad_probs[rows] - mean)).astype(BF16)
        units = pl.ds(chunk * 4, 4)
        value_part = jnp.dot(pbuf[...], grows[group], preferred_element_type=F32)
        key_part = jnp.dot(dsbuf[...], qrows[group], preferred_element_type=F32) * scaling
        for which, found in ((1, value_part), (0, key_part)):
            before = jnp.where(group == 1, 0.0, part[units, which])
            part[units, which] = before + found.reshape(4, SPAN, DIM)
        keys_t = keys.astype(F32).T.astype(BF16)
        dqt[group] += jnp.dot(keys_t, dsbuf[...], preferred_element_type=F32)

        events = (
            (1, 9, reduce_d), (3, 11, reduce_c), (4, 12, reduce_c_opposite), (6, 14, reduce_b),
            (7, 14, reduce_b_along),
        )
        for early, late, event in events:

            @pl.when((step == early) | (step == late))
            def _():
                event(jnp.where(step < 8, 1, 0))

        @pl.when(step == 7)
        def _():
            reduce_a(1)

        @pl.when(step == 10)
        def _():
            for c, slot, sums in own_sums(1):
                put(slot, sums)
                send(stage.at[slot], z_in.at[c], reduce_send, reduce_z, z_other)

        @pl.when(step == 13)
        def _():
            for here, block in query_grads(1):
                dq_out[here, :] = block.astype(BF16)
            send(dq_out, dq_in, dq_send, dq_recv, partner)

        return 0

    lax.fori_loop(0, 16, backward, 0)
    reduce_a(0)
    await_units(reduce_z, 2)
    for c, _, sums in own_sums(0):
        rows = pl.ds(c * SPAN, SPAN)
        dk_ref[rows, :] = (sums[0] + z_in[c, 0].astype(F32)).astype(BF16)
        dv_ref[rows, :] = (sums[1] + z_in[c, 1].astype(F32)).astype(BF16)
    await_units(dq_recv, 4)
    for here, block in query_grads(0):
        dq_ref[here, :] = (block + dq_in[here, :].astype(F32)).astype(BF16)
    await_units(gather_send, 30)
    await_units(q_send, 8)
    await_units(reduce_send, 30)
    await_units(dq_send, 4)
    for group in range(2):
        sent = stats_out.at[group]
        pltpu.make_async_copy(sent, sent, stat_send.at[group]).wait()


def settle(*refs):
    count = len(refs) // 2
    sem = refs[-1]
    copies = [
        pltpu.make_async_copy(source, target, sem.at[i])
        for i, (source, target) in enumerate(zip(refs[:count], refs[count : 2 * count]))
    ]
    for copy in copies:
        copy.start()
    for copy in copies:
        copy.wait()


def settled(*results):
    return pl.pallas_call(
        settle,
        out_shape=tuple(jax.ShapeDtypeStruct(r.shape, r.dtype) for r in results),
        in_specs=[pl.BlockSpec(memory_space=pltpu.VMEM)] * len(results),
        out_specs=tuple([pl.BlockSpec(memory_space=pl.ANY)] * len(results)),
        scratch_shapes=[pltpu.SemaphoreType.DMA((len(results),))],
    )(*(pltpu.with_memory_space_constraint(r, pltpu.VMEM) for r in results))


def local(queries, key_rows, value_slot_rows, out_grad, span_order):
    rows = queries.shape[0]
    vmem = pl.BlockSpec(memory_space=pltpu.VMEM)
    unit = (2, SPAN, DIM)
    dma = pltpu.SemaphoreType.DMA
    dq, dk, dv = pl.pallas_call(
        kernel,
        out_shape=(
            pltpu.VMEM((rows * HEADS, DIM), BF16),
            pltpu.VMEM((rows, DIM), BF16),
            pltpu.VMEM((rows, DIM), BF16),
        ),
        in_specs=[
            pl.BlockSpec(memory_space=pltpu.SMEM),
            *([pl.BlockSpec(memory_space=pl.ANY)] * 4),
        ],
        out_specs=(vmem, vmem, vmem),
        scratch_shapes=[
            pltpu.VMEM((32,) + unit, BF16),
            pltpu.VMEM((32,) + unit, F32),
            pltpu.VMEM((32,) + unit, BF16),
            pltpu.VMEM((32, SPAN, DIM), BF16),
            pltpu.VMEM((2, 3, 2) + unit, BF16),
            pltpu.VMEM((2, 5) + unit, BF16),
            pltpu.VMEM((2,) + unit, BF16),
            pltpu.VMEM((COLS, DIM), BF16),
            pltpu.VMEM((COLS, DIM), BF16),
            pltpu.VMEM((2, 2 * DIM, COLS), BF16),
            pltpu.VMEM((2, DIM, COLS), BF16),
            pltpu.VMEM((2, COLS, DIM), BF16),
            pltpu.VMEM((2, COLS, DIM), BF16),
            pltpu.VMEM((16, 2, CHUNK, SPAN), BF16),
            pltpu.VMEM((16, CHUNK, COLS), F32),
            pltpu.VMEM((CHUNK, COLS), BF16),
            pltpu.VMEM((CHUNK, COLS), BF16),
            pltpu.VMEM((2, DIM, COLS), F32),
            pltpu.VMEM((2, 1, COLS), F32),
            pltpu.VMEM((2, 8, COLS), F32),
            pltpu.VMEM((2, 8, COLS), F32),
            pltpu.VMEM((2, 1, 3 * COLS), F32),
            pltpu.VMEM((2, 1, 3 * COLS), F32),
            pltpu.SMEM((32,), jnp.int32),
            pltpu.SMEM((4,), jnp.int32),
            dma((6,)), dma, dma((2, 10)), dma, dma, dma, dma((2,)), dma((2,)),
            dma, dma((2, 10)), dma, dma, dma,
        ],
        compiler_params=pltpu.CompilerParams(
            collective_id=0, has_side_effects=True, vmem_limit_bytes=60 * 1024 * 1024,
        ),
    )(
        span_order,
        queries.reshape(rows * HEADS, DIM),
        out_grad.reshape(rows * HEADS, DIM),
        key_rows.reshape(rows, DIM),
        value_slot_rows.reshape(rows, DIM),
    )
    dq, dk, dv = settled(dq, dk, dv)
    return (
        dq.reshape(rows, HEADS, DIM),
        dk.reshape(rows, 1, DIM),
        dv.reshape(rows, 1, DIM),
    )


def solution(mesh):
    row = P(("seq", "ctx"), "tp", None)
    return jax.shard_map(
        local,
        mesh=mesh,
        in_specs=(row, row, row, row, P("seq")),
        out_specs=(row, row, row),
        check_vma=False,
    )
```
